128 devices in a mesh: seq: 32 (over x_lo, y, z), tensor: 4 (over x_hi, core).
Axes of the slice: x: 4 (x_hi: 2, x_lo: 2; x = x_hi * 2 + x_lo), y: 4, z: 4, core: 2. Of those that a mesh axis runs over, the one named last changes fastest.
Arguments:
- tokens: bfloat16 [8192, 1024], P('seq'), may hold values from -6 to 6
- w_attn: bfloat16 [2, 1024, 3, 1024], P(None, None, None, 'tensor'), may hold values from -0.1875 to 0.1875
- w_out: bfloat16 [2, 1024, 1024], P(None, None, 'tensor'), may hold values from -0.1875 to 0.1875
- w_up: bfloat16 [2, 1024, 4096], P(None, None, 'tensor'), may hold values from -0.1875 to 0.1875
- w_down: bfloat16 [2, 1024, 4096], P(None, None, 'tensor'), may hold values from -0.09375 to 0.09375
- w_head: bfloat16 [256, 1024], replicated, may hold values from -0.1875 to 0.1875
- gains: float32 [5, 1024], replicated, may hold values from 0.1 to 1.9
- q_cotangent: float32 [8192, 256], P('seq'), may hold values from -0.09 to 0.09
- bounds: int32 [32], P('seq'), may hold values from 1 to 256
- resets: int32 [32], P('seq'), may hold values 0 or 1
Outputs:
- q_values: float32 [8192, 256], P('seq')
- grad_attn: float32 [2, 1024, 3, 1024], P(None, 'seq', None, 'tensor')
- grad_out: float32 [2, 1024, 1024], P(None, 'seq', 'tensor')
- grad_up: float32 [2, 1024, 4096], P(None, 'seq', 'tensor')
- grad_down: float32 [2, 1024, 4096], P(None, 'seq', 'tensor')
- grad_head: float32 [256, 1024], P(None, 'seq')
- grad_gains: float32 [5, 1024], P(None, 'seq')
The draws below stay inside these ranges and needn't reach their ends.
All inputs are finite; a program needn't handle non-finite values. No bound on the sum of `resets` on one device may be relied on, other than what follows from the above.
Results may differ from the reference program's by a relative error of at most 0.033.
Values may be sent and summed in bfloat16 or wider, within the bound.
A program may use at most 128 MiB of HBM per device.

```python
from functools import partial
import jax
import jax.numpy as jnp
from jax import lax

D = 1024
FF = 4096
ACTIONS = 256
LAYERS = 2
SEG = 256
HD = 128
SEGMENTS = 32
TOKENS = 8192


def touch_ends(values, own_key, low, top_value):
    longest = values.shape.index(max(values.shape))
    spots = []
    for shift in (0, 1):
        where = [jax.random.randint(jax.random.fold_in(own_key, axis), (), 0, length) for axis, length in enumerate(values.shape)]
        where[longest] = (where[longest] + shift) % values.shape[longest]
        spots.append(tuple(where))
    return values.at[spots[0]].set(low).at[spots[1]].set(top_value)


def with_spikes(values, stream_key, source, target, parts, factor):
    owner, partner = [(jnp.arange(values.shape[axis_at]) // (values.shape[axis_at] // parts)).reshape([-1 if axis == axis_at else 1 for axis in range(values.ndim)]) for axis_at in (source, target)]
    chosen = jax.random.permutation(stream_key, parts)[partner]
    strong = (owner == chosen) | (owner == (partner + parts // 2) % parts)
    return jnp.where(strong, factor * values, values)


def block_scale(own_key, extent, shards, low, high):
    level = 1.0
    for axis_at, shards_of in shards:
        heights = jax.random.uniform(jax.random.fold_in(jax.random.fold_in(own_key, 6), axis_at), (shards_of,), jnp.float32, low / len(shards), high / len(shards))
        level = level * jnp.repeat(jnp.exp(heights), extent[axis_at] // shards_of).reshape((-1,) + (1,) * (len(extent) - 1 - axis_at))
    return level


def noise(own_key, shape, deviation, most, shards=(), kind=jnp.bfloat16):
    level = block_scale(own_key, shape, shards, -0.22, 0.18) if shards else 1.0
    drawn = jax.random.normal(own_key, shape, jnp.float32) * deviation * level
    return jnp.minimum(jnp.maximum(drawn, -most), most).astype(kind)


def noise_with(stream_key, dims, scale, reach, pieces, heavy, held_as=jnp.bfloat16):
    values = scale * jax.random.normal(stream_key, dims, jnp.float32)
    if pieces:
        values = values * block_scale(stream_key, dims, pieces, -0.22, 0.18)
    return jnp.clip(with_spikes(values, jax.random.fold_in(stream_key, 3), *heavy), -reach, reach).astype(held_as)


def setup_inputs(seed: int = 0) -> dict:
    arg_keys = jax.random.split(jax.random.key(seed), 11)
    return {
        "tokens": noise_with(arg_keys[0], (TOKENS, D), 1.0, 6.0, ((0, 32),), (0, 1, 32, 2.75)),
        "w_attn": noise(arg_keys[1], (LAYERS, D, 3, D), D ** -0.5, 0.1875, ((3, 4),)),
        "w_out": noise(arg_keys[2], (LAYERS, D, D), D ** -0.5, 0.1875, ((2, 4),)),
        "w_up": noise(arg_keys[3], (LAYERS, D, FF), D ** -0.5, 0.1875, ((2, 4),)),
        "w_down": noise(arg_keys[4], (LAYERS, D, FF), FF ** -0.5, 0.09375, ((2, 4),)),
        "w_head": noise(arg_keys[5], (ACTIONS, D), D ** -0.5, 0.1875),
        "gains": jnp.clip(1.0 + 0.18 * jax.random.normal(arg_keys[6], (2 * LAYERS + 1, D), jnp.float32), 0.1, 1.9),
        "q_cotangent": noise(arg_keys[7], (TOKENS, ACTIONS), 0.015625, 0.09, ((0, 32),), jnp.float32),
        "bounds": touch_ends(jax.random.randint(arg_keys[8], (SEGMENTS,), 1, SEG + 1), jax.random.fold_in(arg_keys[8], 1), 1, SEG).astype(jnp.int32),
        "resets": touch_ends((jax.random.randint(arg_keys[9], (SEGMENTS,), 0, 4) < 1).astype(jnp.int32), jax.random.fold_in(arg_keys[9], 1), 0, 1),
    }


epsilon = 1e-06
highest = lax.Precision.HIGHEST

def rms_norm(hidden, gain):
    values = hidden.astype(jnp.float32)
    return values * lax.rsqrt(lax.optimization_barrier(jnp.mean(values * values, axis=-1, keepdims=True)) + epsilon) * gain

def gelu_tanh(up_proj):
    return jax.nn.gelu(up_proj, approximate=True)

def rounded(matrix):
    return lax.optimization_barrier(matrix.astype(jnp.bfloat16)).astype(jnp.float32)

def contract_rows(left, right):
    return lax.dot_general(left, right, (((0,), (0,)), ((), ())), preferred_element_type=jnp.float32)

def contract_cols(left, right):
    return lax.dot_general(left, right, (((1,), (1,)), ((), ())), preferred_element_type=jnp.float32)

def allowed_mask(length, boundary, restart, prior_bound):
    row_ids = lax.broadcasted_iota(jnp.int32, (length, length), 0)
    col_ids = lax.broadcasted_iota(jnp.int32, (length, length), 1)
    before_cut = row_ids < boundary
    own_part = (col_ids <= row_ids) & ((col_ids >= boundary) | before_cut)
    memory_part = before_cut & (restart == 0) & (col_ids >= prior_bound % length)
    return jnp.concatenate([memory_part, own_part], axis=1).astype(jnp.float32)

def project(normed, weights):
    flattened = weights.reshape(weights.shape[0], -1)
    product = jnp.dot(normed, flattened, preferred_element_type=jnp.float32)
    return product.astype(jnp.bfloat16).reshape(normed.shape[0], weights.shape[1], weights.shape[2])

def attend(queries, key_rows, value_rows, allowed):
    scaling = queries.shape[-1] ** (-0.5)
    scores = jnp.einsum('qhd,khd->hqk', queries.astype(jnp.float32), key_rows.astype(jnp.float32), precision=highest) * scaling
    weights = jnp.exp(scores) * allowed[None]
    attn_probs = weights / lax.optimization_barrier(jnp.sum(weights, axis=-1, keepdims=True))
    context = jnp.einsum('hqk,khd->qhd', rounded(attn_probs), value_rows.astype(jnp.float32), precision=highest)
    return (context.astype(jnp.bfloat16), attn_probs)

def attend_back(queries, key_rows, value_rows, attn_probs, d_context):
    scaling = queries.shape[-1] ** (-0.5)
    d_wide = d_context.astype(jnp.float32)
    d_probs = jnp.einsum('qhd,khd->hqk', d_wide, value_rows.astype(jnp.float32), precision=highest)
    d_values = jnp.einsum('hqk,qhd->khd', rounded(attn_probs), d_wide, precision=highest).astype(jnp.bfloat16)
    d_scores = rounded(attn_probs * (d_probs - lax.optimization_barrier(jnp.sum(d_probs * attn_probs, axis=-1, keepdims=True))) * scaling)
    d_queries = jnp.einsum('hqk,khd->qhd', d_scores, key_rows.astype(jnp.float32), precision=highest).astype(jnp.bfloat16)
    d_keys = jnp.einsum('hqk,qhd->khd', d_scores, queries.astype(jnp.float32), precision=highest).astype(jnp.bfloat16)
    return (d_queries, d_keys, d_values)

def layer_forward(hidden, memory, gain_attn, gain_ffn, w_attn, w_out, w_up, w_down, allowed):
    length = hidden.shape[0]
    head_count = w_attn.shape[2] // HD
    normed = rms_norm(hidden, gain_attn).astype(jnp.bfloat16)
    own_proj = project(normed, w_attn)
    mem_proj = project(memory, w_attn[:, 1:])
    queries = own_proj[:, 0].reshape(length, head_count, HD)
    key_rows = jnp.concatenate([mem_proj[:, 0], own_proj[:, 1]], axis=0).reshape(2 * length, head_count, HD)
    value_rows = jnp.concatenate([mem_proj[:, 1], own_proj[:, 2]], axis=0).reshape(2 * length, head_count, HD)
    context, attn_probs = attend(queries, key_rows, value_rows, allowed)
    flat_context = context.reshape(length, -1)
    middle = (hidden.astype(jnp.float32) + contract_cols(flat_context, w_out)).astype(jnp.bfloat16)
    normed_ffn = rms_norm(middle, gain_ffn).astype(jnp.bfloat16)
    up_proj = jnp.dot(normed_ffn, w_up, preferred_element_type=jnp.float32)
    active = gelu_tanh(up_proj).astype(jnp.bfloat16)
    result = (middle.astype(jnp.float32) + contract_cols(active, w_down)).astype(jnp.bfloat16)
    stored = (normed, queries, key_rows, value_rows, attn_probs, flat_context, middle, normed_ffn, up_proj, active)
    return (result, stored)

def layer_backward(hidden, memory, stored, gain_attn, gain_ffn, w_attn, w_out, w_up, w_down, d_result):
    normed, queries, key_rows, value_rows, attn_probs, flat_context, middle, normed_ffn, up_proj, active = stored
    length, features = hidden.shape
    d_ffn = d_result.astype(jnp.bfloat16)
    grad_down = contract_rows(d_ffn, active)
    d_active = jnp.dot(d_ffn, w_down, preferred_element_type=jnp.float32)
    d_upper = jax.vjp(gelu_tanh, up_proj)[1](d_active)[0].astype(jnp.bfloat16)
    grad_up = contract_rows(normed_ffn, d_upper)
    d_normed_ffn = contract_cols(d_upper, w_up)
    d_mid_norm, grad_gain_ffn = jax.vjp(rms_norm, middle.astype(jnp.float32), gain_ffn)[1](d_normed_ffn)
    d_middle = d_result + d_mid_norm
    d_attn = d_middle.astype(jnp.bfloat16)
    grad_out = contract_rows(d_attn, flat_context)
    d_context = jnp.dot(d_attn, w_out, preferred_element_type=jnp.float32).astype(jnp.bfloat16).reshape(queries.shape)
    d_queries, d_keys, d_values = attend_back(queries, key_rows, value_rows, attn_probs, d_context)
    d_own = jnp.stack([d_queries.reshape(length, -1), d_keys[length:].reshape(length, -1), d_values[length:].reshape(length, -1)], axis=1)
    d_mem = jnp.stack([d_keys[:length].reshape(length, -1), d_values[:length].reshape(length, -1)], axis=1)
    grad_attn = contract_rows(normed, d_own.reshape(length, -1)).reshape(w_attn.shape)
    mem_term = contract_rows(memory, d_mem.reshape(length, -1)).reshape(features, 2, -1)
    grad_attn = grad_attn.at[:, 1:].add(mem_term)
    d_normed = contract_cols(d_own.reshape(length, -1), w_attn.reshape(features, -1))
    d_hid_norm, grad_gain_attn = jax.vjp(rms_norm, hidden.astype(jnp.float32), gain_attn)[1](d_normed)
    return (d_middle + d_hid_norm, (grad_attn, grad_out, grad_up, grad_down), (grad_gain_attn, grad_gain_ffn))

def advance(params, layer_idx, operands):
    w_attn, w_out, w_up, w_down, w_head, gains = params
    seg_hidden, seg_memory, allowed = operands
    return layer_forward(seg_hidden, seg_memory, gains[2 * layer_idx], gains[2 * layer_idx + 1], w_attn[layer_idx], w_out[layer_idx], w_up[layer_idx], w_down[layer_idx], allowed)[0]

def segment_grads(params, totals, operands):
    w_attn, w_out, w_up, w_down, w_head, gains = params
    seg_inputs, seg_memories, allowed, seg_cotangent, top_hidden = operands
    stores = []
    for layer_idx in range(LAYERS):
        stores.append(layer_forward(seg_inputs[layer_idx], seg_memories[layer_idx], gains[2 * layer_idx], gains[2 * layer_idx + 1], w_attn[layer_idx], w_out[layer_idx], w_up[layer_idx], w_down[layer_idx], allowed)[1])
    final_norm = rms_norm(top_hidden, gains[2 * LAYERS]).astype(jnp.bfloat16)
    d_actions = seg_cotangent.astype(jnp.bfloat16)
    grad_head = contract_rows(d_actions, final_norm)
    d_final = jnp.dot(d_actions, w_head, preferred_element_type=jnp.float32)
    d_hidden, grad_gain_top = jax.vjp(rms_norm, top_hidden.astype(jnp.float32), gains[2 * LAYERS])[1](d_final)
    layer_grads = [None] * LAYERS
    gain_grads = [None] * (2 * LAYERS)
    for layer_idx in reversed(range(LAYERS)):
        d_hidden, layer_grads[layer_idx], gain_pair = layer_backward(seg_inputs[layer_idx], seg_memories[layer_idx], stores[layer_idx], gains[2 * layer_idx], gains[2 * layer_idx + 1], w_attn[layer_idx], w_out[layer_idx], w_up[layer_idx], w_down[layer_idx], d_hidden)
        gain_grads[2 * layer_idx] = gain_pair[0]
        gain_grads[2 * layer_idx + 1] = gain_pair[1]
    stacked = [jnp.stack([layer_grads[level_idx][member] for level_idx in range(LAYERS)]) for member in range(4)]
    updated = (totals[0] + stacked[0], totals[1] + stacked[1], totals[2] + stacked[2], totals[3] + stacked[3], totals[4] + grad_head, totals[5] + jnp.stack(gain_grads + [grad_gain_top]))
    return (updated, None)

def reference(tokens, w_attn, w_out, w_up, w_down, w_head, gains, q_cotangent, bounds, resets):
    segments = bounds.shape[0]
    length = tokens.shape[0] // segments
    features = tokens.shape[1]
    params = (w_attn, w_out, w_up, w_down, w_head, gains)
    first_flag = (jnp.arange(segments, dtype=jnp.int32) == 0).astype(jnp.int32)
    restarts = jnp.maximum(resets, first_flag)
    prior_bounds = jnp.roll(bounds, 1)
    masks = lax.map(lambda flags: allowed_mask(length, flags[0], flags[1], flags[2]), (bounds, restarts, prior_bounds))
    hidden = tokens.reshape(segments, length, features)
    layer_inputs = []
    layer_memories = []
    for layer_idx in range(LAYERS):
        memory = jnp.roll(rms_norm(hidden, gains[2 * layer_idx]).astype(jnp.bfloat16), 1, axis=0)
        memory = memory.at[0].set(jnp.zeros((length, features), jnp.bfloat16))
        layer_inputs.append(hidden)
        layer_memories.append(memory)
        hidden = lax.map(partial(advance, params, layer_idx), (hidden, memory, masks))
    final_norm = rms_norm(hidden, gains[2 * LAYERS]).astype(jnp.bfloat16)
    q_values = contract_cols(final_norm.reshape(-1, features), w_head)
    start = (jnp.zeros(w_attn.shape, jnp.float32), jnp.zeros(w_out.shape, jnp.float32), jnp.zeros(w_up.shape, jnp.float32), jnp.zeros(w_down.shape, jnp.float32), jnp.zeros(w_head.shape, jnp.float32), jnp.zeros(gains.shape, jnp.float32))
    operands = (tuple(layer_inputs), tuple(layer_memories), masks, q_cotangent.reshape(segments, length, -1), hidden)
    totals, _ = lax.scan(partial(segment_grads, params), start, operands)
    return (q_values, totals[0], totals[1], totals[2], totals[3], totals[4], totals[5])
```

```python
import functools
import types

import jax
import jax.numpy as jnp
from jax import lax
from jax.experimental import pallas as pl
from jax.experimental.pallas import tpu as pltpu
from jax.sharding import PartitionSpec as P

F32 = jnp.float32
BF16 = jnp.bfloat16
EPS = 1e-06
LAYERS = 2
D = 1024
SEG = 256
HD = 128
CUBIC = 0.044715
ROOT = 0.7978845608028654
MESH = pl.DeviceIdType.MESH
UNITS = 24
NARROW = 3


def nn(a, b):
    return lax.dot_general(a, b, (((1,), (0,)), ((), ())), preferred_element_type=F32)


def nt(a, b):
    return lax.dot_general(a, b, (((1,), (1,)), ((), ())), preferred_element_type=F32)


def tn(a, b):
    return lax.dot_general(a, b, (((0,), (0,)), ((), ())), preferred_element_type=F32)


def loop(count, f):
    def step(i, carry):
        f(i)
        return carry

    lax.fori_loop(0, count, step, 0)


def span(i, size):
    return pl.ds(pl.multiple_of(i * size, size), size)


def near(v):
    return v + 1 - 2 * lax.rem(v, 2)


def far(v):
    return 3 - v


INPUTS = ("tokens", "wa", "wo", "wu", "wd", "wh", "gains", "qcot", "bound", "reset")
OUTPUTS = ("oz", "oe")


def scratch():
    v = pltpu.VMEM
    dma = pltpu.SemaphoreType.DMA
    return dict(
        wA=v((2, 3, D, 256), BF16),
        wO=v((2, D, 256), BF16),
        wU=v((2, D, D), BF16),
        wD=v((2, D, D), BF16),
        wH=v((256, D), BF16),
        h=v((3, SEG, D), BF16),
        a=v((2, 2 * SEG, D), BF16),
        q=v((2, SEG, 256), BF16),
        k=v((2, 2 * SEG, 256), BF16),
        v=v((2, 2 * SEG, 256), BF16),
        p=v((2, 2, SEG, 2 * SEG), F32),
        ctx=v((2, SEG, 256), BF16),
        mid=v((2, SEG, D), BF16),
        b=v((2, SEG, D), BF16),
        slope=v((2, SEG, D), F32),
        act=v((2, SEG, D), BF16),
        ar_send=v((128, D), BF16),
        ar_half=v((2, 128, D), BF16),
        ar_sum=v((128, D), BF16),
        ar_far=v((2, 128, D), BF16),
        ar_own=v((128, D), F32),
        db=v((SEG, D), BF16),
        dh=v((SEG, D), F32),
        xt=v((D, 2 * SEG), BF16),
        final=v((SEG, D), BF16),
        dy=v((SEG, D), BF16),
        dup=v((SEG, D), BF16),
        dctx=v((SEG, 256), BF16),
        dqs=v((SEG, 256), BF16),
        dkv=v((2, 2 * SEG, 256), BF16),
        wide_tmp=v((SEG, D), F32),
        gg=v((5, 8, D), F32),
        g0=v((2, 8, D), F32),
        g0s=v((8, D), F32),
        bs=v((8, 256), jnp.int32),
        br=v((8, 256), jnp.int32),
        G=v((UNITS, 2, 4, 4, 32, 256), BF16),
        R1=v((UNITS, 2, 2, 4, 32, 256), BF16),
        R2=v((UNITS, 2, 4, 32, 256), BF16),
        R3=v((UNITS, 2, 2, 32, 256), BF16),
        R4=v((UNITS, 2, 32, 256), BF16),
        R5=v((UNITS, 32, 256), BF16),
        G_=v((NARROW, 2, 4, 4, 32, 128), BF16),
        R1_=v((NARROW, 2, 2, 4, 32, 128), BF16),
        R2_=v((NARROW, 2, 4, 32, 128), BF16),
        R3_=v((NARROW, 2, 2, 32, 128), BF16),
        R4_=v((NARROW, 2, 32, 128), BF16),
        R5_=v((NARROW, 32, 128), BF16),
        w_sem=dma((10,)),
        ar_s=dma((7, 3)),
        ar_r=dma((7, 3)),
        kv_s=dma((2, 2)),
        kv_r=dma((2, 2)),
        pa_s=dma((2, 2)),
        pa_r=dma((2, 2)),
        b_s=dma,
        b_r=dma,
        g0_s=dma((2,)),
        g0_r=dma((2,)),
        rs_s=dma((UNITS + NARROW, 7)),
        rs_r=dma((UNITS + NARROW, 7)),
    )


COLORS = (("y", 0, 0), ("z", 0, 0), ("y", 1, 1), ("z", 1, 1))


class Share:
    def __init__(self, r, here, index, narrow, color, write):
        tail = "_" if narrow else ""
        self.g, self.r1, self.r2, self.r3, self.r4, self.r5 = (
            getattr(r, name + tail).at[index] for name in ("G", "R1", "R2", "R3", "R4", "R5")
        )
        row = index + (UNITS if narrow else 0)
        self.ss = [r.rs_s.at[row, n] for n in range(7)]
        self.rs = [r.rs_r.at[row, n] for n in range(7)]
        self.here = here
        self.axis, o1, o2 = color
        self.f1, self.f2 = (far, near) if o1 else (near, far)
        self.e1, self.e2 = (far, near) if o2 else (near, far)
        self.write = write
        self.stage = 0

    def one(self, value):
        return self.g.at[:, value] if self.axis == "y" else self.g.at[:, :, value]

    def two(self, value):
        if self.axis == "y":
            return self.g.at[:, self.here.y, value]
        return self.g.at[:, value, self.here.z]

    def device(self, first=None, second=None, x=None):
        h = self.here
        y, z = h.y, h.z
        if first is not None:
            y, z = (first, z) if self.axis == "y" else (y, first)
        if second is not None:
            y, z = (y, second) if self.axis == "y" else (second, z)
        x = h.x if x is None else x
        return (x * 16 + y * 4 + z, h.t)

    def send(self, n, source, target, device):
        copy = pltpu.make_async_remote_copy(
            src_ref=source,
            dst_ref=target,
            send_sem=self.ss[n],
            recv_sem=self.rs[n],
            device_id=device,
            device_id_type=MESH,
        )
        copy.start()
        return copy

    def advance(self):
        h = self.here
        v, w = (h.y, h.z) if self.axis == "y" else (h.z, h.y)
        stage = self.stage
        if stage > 5:
            return
        self.stage += 1
        if stage == 0:
            peer = self.f1(v)
            to = self.device(first=peer)
            self.c = [
                self.send(0, self.one(peer), self.r1.at[0], to),
                self.send(1, self.one(self.f2(peer)), self.r1.at[1], to),
            ]
            return
        for copy in self.c:
            copy.wait()
        if stage == 1:
            peer = self.f2(v)
            part = self.one(peer)
            part[...] = (part[...].astype(F32) + self.r1[1].astype(F32)).astype(BF16)
            self.c = [self.send(2, part, self.r2, self.device(first=peer))]
        elif stage == 2:
            part = self.one(v)
            part[...] = (
                part[...].astype(F32) + self.r1[0].astype(F32) + self.r2[...].astype(F32)
            ).astype(BF16)
            peer = self.e1(w)
            to = self.device(second=peer)
            self.c = [
                self.send(3, self.two(peer), self.r3.at[0], to),
                self.send(4, self.two(self.e2(peer)), self.r3.at[1], to),
            ]
        elif stage == 3:
            peer = self.e2(w)
            part = self.two(peer)
            part[...] = (part[...].astype(F32) + self.r3[1].astype(F32)).astype(BF16)
            self.c = [self.send(5, part, self.r4, self.device(second=peer))]
        elif stage == 4:
            part = self.two(w)
            part[...] = (
                part[...].astype(F32) + self.r3[0].astype(F32) + self.r4[...].astype(F32)
            ).astype(BF16)
            other = self.g.at[1 - h.x, h.y, h.z]
            self.c = [self.send(6, other, self.r5, self.device(x=1 - h.x))]
        else:
            own = self.g[h.x, h.y, h.z]
            self.write(own.astype(F32) + self.r5[...].astype(F32))


def norm_vjp(x, gain, dy):
    r = lax.rsqrt(jnp.mean(x * x, axis=-1, keepdims=True) + EPS)
    scaled = dy * gain
    inner = jnp.mean(scaled * x, axis=-1, keepdims=True)
    dx = r * scaled - x * (r * r * r * inner)
    return dx, dy * (x * r)


def kernel(*refs):
    scratches = scratch()
    r = types.SimpleNamespace(**dict(zip(INPUTS + OUTPUTS + tuple(scratches), refs)))
    s = lax.axis_index("seq")
    t = lax.axis_index("tensor")
    here = types.SimpleNamespace(
        x=lax.div(s, 16), y=lax.rem(lax.div(s, 4), 4), z=lax.rem(s, 4), t=t, s=s
    )
    core, chip = lax.rem(t, 2), lax.div(t, 2)
    beside = (s, chip * 2 + 1 - core)
    across = (s, (1 - chip) * 2 + core)
    following = (lax.rem(s + 1, 32), t)
    preceding = (lax.rem(s + 31, 32), t)
    at = lambda x, y, z: (x * 16 + y * 4 + z, t)
    peers = [
        beside,
        across,
        following,
        preceding,
        at(1 - here.x, here.y, here.z),
        at(here.x, near(here.y), here.z),
        at(here.x, far(here.y), here.z),
        at(here.x, here.y, near(here.z)),
        at(here.x, here.y, far(here.z)),
    ]

    loads = {}
    order = [("tok", r.tokens, r.h.at[0])]
    for l in range(LAYERS):
        order.append((("A", l), r.wa.at[l], r.wA.at[l]))
        order.append((("O", l), r.wo.at[l], r.wO.at[l]))
        order.append((("U", l), r.wu.at[l], r.wU.at[l]))
        order.append((("D", l), r.wd.at[l], r.wD.at[l]))
    order.append(("H", r.wh, r.wH))
    for n, (name, source, target) in enumerate(order):
        loads[name] = pltpu.make_async_copy(source, target, r.w_sem.at[n])
        if n < 2:
            loads[name].start()

    barrier = pltpu.get_barrier_semaphore()
    for peer in peers:
        pl.semaphore_signal(barrier, inc=1, device_id=peer, device_id_type=MESH)
    r.gg[...] = jnp.zeros_like(r.gg)
    bound = r.bound[0]
    restart = jnp.where(s == 0, 1, r.reset[0])
    r.bs[...] = jnp.full((8, 256), bound, jnp.int32)

    def remote(source, target, send_sem, recv_sem, device):
        return pltpu.make_async_remote_copy(
            src_ref=source,
            dst_ref=target,
            send_sem=send_sem,
            recv_sem=recv_sem,
            device_id=device,
            device_id_type=MESH,
        )

    def norm_into(source, k, target):
        def rows(i):
            block = span(i, 64)
            x = source[block, :].astype(F32)
            scale = lax.rsqrt(jnp.mean(x * x, axis=-1, keepdims=True) + EPS)
            target[block, :] = (x * scale * r.gains[k : k + 1, :]).astype(BF16)

        loop(4, rows)

    def ar_begin(n, part):
        base = (1 - core) * 128

        def first(i):
            r.ar_send[:, span(i, 256)] = part(base, i).astype(BF16)

        loop(4, first)
        half = r.ar_half.at[n % 2]
        copy = remote(r.ar_send, half, r.ar_s.at[n, 0], r.ar_r.at[n, 0], beside)
        copy.start()

        def second(i):
            r.ar_own[:, span(i, 256)] = part(core * 128, i)

        loop(4, second)
        copy.wait()
        r.ar_sum[...] = (r.ar_own[...] + half[...].astype(F32)).astype(BF16)
        copy = remote(
            r.ar_sum, r.ar_far.at[n % 2], r.ar_s.at[n, 1], r.ar_r.at[n, 1], across
        )
        copy.start()
        return copy

    def ar_end(n, copy, target, residual):
        copy.wait()
        mine = pl.ds(pl.multiple_of(core * 128, 128), 128)
        total = r.ar_sum[...].astype(F32) + r.ar_far[n % 2].astype(F32)
        if residual is not None:
            total = residual[mine, :].astype(F32) + total
        target[mine, :] = total.astype(BF16)
        copy = remote(
            target.at[mine, :], target.at[mine, :], r.ar_s.at[n, 2], r.ar_r.at[n, 2], beside
        )
        copy.start()
        copy.wait()

    def at_rows(base):
        return pl.ds(pl.multiple_of(base, 128), 128)

    loads["tok"].wait()
    own = pl.ds(SEG, SEG)
    for l in range(LAYERS):
        h, a, q, k, v = r.h.at[l], r.a.at[l, own], r.q.at[l], r.k.at[l], r.v.at[l]
        norm_into(h, 2 * l, a)
        loads["A", l].wait()
        if l == 0:
            for name, _, _ in order[2:]:
                loads[name].start()
        k[own, :] = nn(a[...], r.wA[l, 1]).astype(BF16)
        if l == 0:
            pl.semaphore_wait(barrier, len(peers))
            bound_copy = remote(r.bs, r.br, r.b_s, r.b_r, following)
            bound_copy.start()
        send_k = remote(
            k.at[own], k.at[pl.ds(0, SEG)], r.kv_s.at[l, 0], r.kv_r.at[l, 0], following
        )
        send_k.start()
        v[own, :] = nn(a[...], r.wA[l, 2]).astype(BF16)
        send_v = remote(
            v.at[own], v.at[pl.ds(0, SEG)], r.kv_s.at[l, 1], r.kv_r.at[l, 1], following
        )
        send_v.start()
        q[...] = nn(a[...], r.wA[l, 0]).astype(BF16)
        for head in range(2):
            lanes = slice(head * HD, (head + 1) * HD)

            def local(i):
                block = span(i, 128)
                scores = nt(q[block, lanes], k[own, lanes]) * (HD**-0.5)
                row = lax.broadcasted_iota(jnp.int32, (128, SEG), 0) + i * 128
                col = lax.broadcasted_iota(jnp.int32, (128, SEG), 1)
                allowed = (col <= row) & ((col >= bound) | (row < bound))
                r.p[l, head, block, own] = jnp.where(allowed, jnp.exp(scores), 0.0)

            loop(2, local)
        if l == 0:
            bound_copy.wait()
        send_k.wait()
        for head in range(2):
            lanes = slice(head * HD, (head + 1) * HD)

            def memory(i):
                block = span(i, 128)
                scores = nt(q[block, lanes], k[0:SEG, lanes]) * (HD**-0.5)
                row = lax.broadcasted_iota(jnp.int32, (128, SEG), 0) + i * 128
                col = lax.broadcasted_iota(jnp.int32, (128, SEG), 1)
                prior = lax.rem(r.br[0:1, :], SEG)
                allowed = (row < bound) & (restart == 0) & (col >= prior)
                e = jnp.where(allowed, jnp.exp(scores), 0.0)
                e_own = r.p[l, head, block, own]
                total = jnp.sum(e + e_own, axis=-1, keepdims=True)
                r.p[l, head, block, 0:SEG] = e / total
                r.p[l, head, block, own] = e_own / total

            loop(2, memory)
        send_v.wait()
        prev = r.a.at[l, at_rows(core * 128)]
        send_a = remote(
            r.a.at[l, at_rows(SEG + core * 128)],
            prev,
            r.pa_s.at[l, 0],
            r.pa_r.at[l, 0],
            following,
        )
        send_a.start()
        for head in range(2):
            lanes = slice(head * HD, (head + 1) * HD)

            def attend(i):
                block = span(i, 128)
                probs = r.p[l, head, block, :].astype(BF16)
                r.ctx[l, block, lanes] = nn(probs, v[:, lanes]).astype(BF16)

            loop(2, attend)
        loads["O", l].wait()
        copy = ar_begin(
            2 * l, lambda base, i: nt(r.ctx[l, at_rows(base), :], r.wO[l, span(i, 256), :])
        )
        ar_end(2 * l, copy, r.mid.at[l], h)
        norm_into(r.mid.at[l], 2 * l + 1, r.b.at[l])
        loads["U", l].wait()

        def upper(i):
            lanes = span(i, 256)
            u = nn(r.b[l], r.wU[l, :, lanes])
            th = jnp.tanh(ROOT * (u + CUBIC * (u * u * u)))
            half = 0.5 * (1.0 + th)
            r.act[l, :, lanes] = (u * half).astype(BF16)
            r.slope[l, :, lanes] = half + (0.5 * ROOT) * u * (1.0 - th * th) * (
                1.0 + (3.0 * CUBIC) * (u * u)
            )

        loop(4, upper)
        loads["D", l].wait()
        copy = ar_begin(
            2 * l + 1,
            lambda base, i: nt(r.act[l, at_rows(base), :], r.wD[l, span(i, 256), :]),
        )
        send_a.wait()
        share_a = remote(prev, prev, r.pa_s.at[l, 1], r.pa_r.at[l, 1], beside)
        share_a.start()
        ar_end(2 * l + 1, copy, r.h.at[l + 1], r.mid.at[l])
        share_a.wait()

    def transposed(source):
        count = source.shape[0]

        def cols(i):
            lanes = span(i, 256)
            r.xt[lanes, 0:count] = source[:, lanes].T

        loop(4, cols)

    def outer(g, value):
        g[...] = value.astype(BF16).reshape(g.shape)

    def share(index, narrow, color, write):
        return Share(r, here, index, narrow, COLORS[color], write)

    def wide(index, color, left, write):
        unit = share(index, False, color, write)
        outer(unit.g, left())
        unit.advance()
        return unit

    def step(units):
        for unit in units:
            unit.advance()

    def norm_back(source, k, dy_of, add):
        def rows(i):
            block = span(i, 64)
            dx, dg = norm_vjp(source[block, :].astype(F32), r.gains[k : k + 1, :], dy_of(block))
            r.dh[block, :] = (r.dh[block, :] + dx) if add else dx
            r.gg[k] += jnp.sum(dg.reshape(8, 8, D), axis=0)

        loop(4, rows)

    def rounded_dh():
        def rows(i):
            block = span(i, 64)
            r.dy[block, :] = r.dh[block, :].astype(BF16)

        loop(4, rows)

    dq = r.dctx
    loads["H"].wait()
    dq[...] = r.qcot[...].astype(BF16)

    def top(i):
        lanes = span(i, 256)
        r.wide_tmp[:, lanes] = nn(dq[...], r.wH[:, lanes])

    loop(4, top)
    norm_back(r.h.at[2], 4, lambda block: r.wide_tmp[block, :], False)

    def head_grads():
        norm_into(r.h.at[2], 4, r.final)
        r.oe[0:256, :] = nt(r.final[...], r.wH[...])
        transposed(r.final)
        units = []
        for n in range(2):

            def write(value, n=n):
                r.oe[256:288, n * 128 : (n + 1) * 128] = value

            unit = share(n, True, n, write)
            outer(unit.g, nn(r.xt[:, 0:SEG], dq[:, n * 128 : (n + 1) * 128]))
            unit.advance()
            units.append(unit)
        return units

    def ffn_back(l, n):
        rounded_dh()

        def gate(i):
            lanes = span(i, 256)
            d_active = nn(r.dy[...], r.wD[l, :, lanes])
            r.dup[:, lanes] = (d_active * r.slope[l, :, lanes]).astype(BF16)

        loop(4, gate)
        return ar_begin(
            n, lambda base, i: nt(r.dup[at_rows(base), :], r.wU[l, span(i, 256), :])
        )

    def ffn_grads(l):
        units = []
        for kind, (left, right, out) in enumerate(
            ((r.dy, r.act.at[l], 1024), (r.b.at[l], r.dup, 0))
        ):
            transposed(left)
            for n in range(4):

                def write(value, base=out + n * 256):
                    r.oz[l, :, base : base + 256] = value

                units.append(
                    wide(
                        l * 12 + kind * 4 + n,
                        n,
                        lambda n=n, right=right: nn(
                            r.xt[:, 0:SEG], right[:, n * 256 : (n + 1) * 256]
                        ),
                        write,
                    )
                )
        return units

    def attention_back(l):
        norm_back(r.mid.at[l], 2 * l + 1, lambda block: r.db[block, :].astype(F32), True)
        rounded_dh()
        r.dctx[...] = nn(r.dy[...], r.wO[l]).astype(BF16)
        q, k, v = r.q.at[l], r.k.at[l], r.v.at[l]
        for head in range(2):
            lanes = slice(head * HD, (head + 1) * HD)
            d = r.dctx[:, lanes]
            probs = r.p[l, head]
            d_probs = nt(d, v[:, lanes])
            inner = jnp.sum(d_probs * probs, axis=-1, keepdims=True)
            d_scores = (probs * (d_probs - inner) * (HD**-0.5)).astype(BF16)
            r.dqs[:, lanes] = nn(d_scores, k[:, lanes]).astype(BF16)
            r.dkv[0, :, lanes] = tn(d_scores, q[:, lanes]).astype(BF16)
            r.dkv[1, :, lanes] = tn(probs.astype(BF16), d).astype(BF16)

    def unit_index(l, n):
        return l * 12 + 8 + n

    def out_grads(l):
        transposed(r.dy)

        def write(value):
            r.oz[l, :, 2048:2304] = value

        return [wide(unit_index(l, 3), 3, lambda: nn(r.xt[:, 0:SEG], r.ctx[l]), write)]

    def qkv_grads(l):
        transposed(r.a.at[l])
        units = []
        for n in range(3):

            def write(value, base=2304 + n * 256):
                r.oz[l, :, base : base + 256] = value

            def left(n=n):
                if n:
                    return nn(r.xt[...], r.dkv[n - 1])
                return nn(r.xt[:, SEG:], r.dqs[...])

            units.append(wide(unit_index(l, n), n, left, write))
        return units

    def back_part(l):
        def part(base, i):
            total = nt(r.dqs[at_rows(base), :], r.wA[l, 0, span(i, 256), :])
            for n in (1, 2):
                total = total + nt(
                    r.dkv[n - 1, at_rows(SEG + base), :], r.wA[l, n, span(i, 256), :]
                )
            return total

        return part

    copy = ffn_back(1, 4)
    ffn1 = ffn_grads(1)
    heads = head_grads()
    ar_end(4, copy, r.db, None)
    attention_back(1)
    copy = ar_begin(5, back_part(1))
    step(ffn1)
    step(heads)
    attn1 = out_grads(1) + qkv_grads(1)
    ar_end(5, copy, r.db, None)
    norm_back(r.h.at[1], 2, lambda block: r.db[block, :].astype(F32), True)
    copy = ffn_back(0, 6)
    step(ffn1)
    step(heads)
    step(attn1)
    ffn0 = ffn_grads(0)
    ar_end(6, copy, r.db, None)
    attention_back(0)
    attn0 = out_grads(0) + qkv_grads(0)
    step(heads)
    step(ffn1)
    step(attn1)

    def normal(i):
        block = span(i, 64)
        x = r.h[0, block, :].astype(F32)
        r.dh[block, :] = x * lax.rsqrt(jnp.mean(x * x, axis=-1, keepdims=True) + EPS)

    loop(4, normal)
    part = back_part(0)
    for half in range(2):

        def gain(i):
            lanes = span(i, 256)
            rows = pl.ds(half * 128, 128)
            value = part(half * 128, i) * r.dh[rows, lanes]
            r.gg[0, :, lanes] += jnp.sum(value.reshape(16, 8, 256), axis=0)

        loop(4, gain)
    copy = remote(r.gg.at[0], r.g0.at[0], r.g0_s.at[0], r.g0_r.at[0], beside)
    copy.start()
    copy.wait()
    r.g0s[...] = r.gg[0] + r.g0[0]
    copy = remote(r.g0s, r.g0.at[1], r.g0_s.at[1], r.g0_r.at[1], across)
    copy.start()
    step(heads)
    step(ffn1)
    step(attn1)
    step(ffn0)
    copy.wait()
    rows = [jnp.sum(r.g0s[...] + r.g0[1], axis=0, keepdims=True)]
    rows += [jnp.sum(r.gg[n], axis=0, keepdims=True) for n in range(1, 5)]
    table = jnp.concatenate(rows + [jnp.zeros((123, D), F32)], axis=0)

    def write_gains(value):
        r.oe[288:320, 0:128] = value

    unit = share(2, True, 3, write_gains)
    outer(unit.g, table.T)
    unit.advance()
    step(attn0)
    tail = attn0 + [unit]
    for n in range(2, 7):
        step(heads)
        step(ffn1)
        step(attn1)
        step(ffn0)
        step(tail)


def body(tokens, w_attn, w_out, w_up, w_down, w_head, gains, q_cotangent, bounds, resets):
    vmem = pl.BlockSpec(memory_space=pltpu.VMEM)
    smem = pl.BlockSpec(memory_space=pltpu.SMEM)
    anywhere = pl.BlockSpec(memory_space=pl.ANY)
    shapes = [(2, 32, 3072), (320, 256)]
    outs = pl.pallas_call(
        kernel,
        out_shape=[jax.ShapeDtypeStruct(shape, F32) for shape in shapes],
        in_specs=[anywhere] * 6 + [vmem] * 2 + [smem] * 2,
        out_specs=[vmem] * len(shapes),
        scratch_shapes=list(scratch().values()),
        compiler_params=pltpu.CompilerParams(
            collective_id=0, has_side_effects=True, vmem_limit_bytes=67043328
        ),
    )(
        tokens,
        jnp.transpose(w_attn, (0, 2, 1, 3)),
        w_out,
        w_up,
        w_down,
        w_head,
        gains,
        q_cotangent,
        bounds,
        resets,
    )
    grads, rest = outs
    return (
        rest[:256],
        grads[:, :, 2304:].reshape(2, 32, 3, 256),
        grads[:, :, 2048:2304],
        grads[:, :, :1024],
        grads[:, :, 1024:2048],
        rest[256:288].T,
        rest[288:320, :5].T,
    )


def solution(mesh):
    return jax.shard_map(
        body,
        mesh=mesh,
        in_specs=(
            P("seq", None),
            P(None, None, None, "tensor"),
            P(None, None, "tensor"),
            P(None, None, "tensor"),
            P(None, None, "tensor"),
            P(),
            P(),
            P("seq", None),
            P("seq"),
            P("seq"),
        ),
        out_specs=(
            P("seq", None),
            P(None, "seq", None, "tensor"),
            P(None, "seq", "tensor"),
            P(None, "seq", "tensor"),
            P(None, "seq", "tensor"),
            P(None, "seq"),
            P(None, "seq"),
        ),
        check_vma=False,
    )
```

```python
import functools
import types

import jax
import jax.numpy as jnp
from jax import lax
from jax.experimental import pallas as pl
from jax.experimental.pallas import tpu as pltpu
from jax.sharding import PartitionSpec as P

F32 = jnp.float32
BF16 = jnp.bfloat16
EPS = 1e-06
LAYERS = 2
D = 1024
SEG = 256
HD = 128
CUBIC = 0.044715
ROOT = 0.7978845608028654
MESH = pl.DeviceIdType.MESH
UNITS = 24
NARROW = 3


def nn(a, b):
    return lax.dot_general(a, b, (((1,), (0,)), ((), ())), preferred_element_type=F32)


def nt(a, b):
    return lax.dot_general(a, b, (((1,), (1,)), ((), ())), preferred_element_type=F32)


def tn(a, b):
    return lax.dot_general(a, b, (((0,), (0,)), ((), ())), preferred_element_type=F32)


def loop(count, f):
    def step(i, carry):
        f(i)
        return carry

    lax.fori_loop(0, count, step, 0)


def span(i, size):
    if isinstance(i, int):
        return pl.ds(i * size, size)
    return pl.ds(pl.multiple_of(i * size, size), size)


def near(v):
    return v + 1 - 2 * lax.rem(v, 2)


def far(v):
    return 3 - v


INPUTS = ("tokens", "wa", "wo", "wu", "wd", "wh", "gains", "qcot", "bound", "reset")
OUTPUTS = ("oz", "oe")


def scratch():
    v = pltpu.VMEM
    dma = pltpu.SemaphoreType.DMA
    return dict(
        wA=v((2, 3, D, 256), BF16),
        wO=v((2, D, 256), BF16),
        wU=v((2, D, D), BF16),
        wD=v((2, D, D), BF16),
        wH=v((256, D), BF16),
        h=v((3, SEG, D), BF16),
        a=v((2, 2 * SEG, D), BF16),
        q=v((2, SEG, 256), BF16),
        k=v((2, 2 * SEG, 256), BF16),
        v=v((2, 2 * SEG, 256), BF16),
        p=v((2, 2, SEG, 2 * SEG), F32),
        ctx=v((2, SEG, 256), BF16),
        mid=v((2, SEG, D), BF16),
        b=v((2, SEG, D), BF16),
        slope=v((2, SEG, D), F32),
        act=v((2, SEG, D), BF16),
        ar_send=v((128, D), BF16),
        ar_half=v((2, 128, D), BF16),
        ar_sum=v((128, D), BF16),
        ar_far=v((2, 128, D), BF16),
        db=v((SEG, D), BF16),
        dh=v((SEG, D), F32),
        xt=v((D, 2 * SEG), BF16),
        final=v((SEG, D), BF16),
        dy=v((SEG, D), BF16),
        dup=v((SEG, D), BF16),
        dctx=v((SEG, 256), BF16),
        dqs=v((SEG, 256), BF16),
        dkv=v((2, 2 * SEG, 256), BF16),
        wide_tmp=v((SEG, D), F32),
        gg=v((5, 8, D), F32),
        g0=v((2, 8, D), F32),
        g0s=v((8, D), F32),
        bs=v((8, 256), jnp.int32),
        br=v((8, 256), jnp.int32),
        G=v((UNITS, 2, 4, 4, 32, 256), BF16),
        R1=v((UNITS, 2, 2, 4, 32, 256), BF16),
        R2=v((UNITS, 2, 4, 32, 256), BF16),
        R3=v((UNITS, 3, 2, 32, 256), BF16),
        R5=v((UNITS, 32, 256), BF16),
        G_=v((NARROW, 2, 4, 4, 32, 128), BF16),
        R1_=v((NARROW, 3, 2, 4, 32, 128), BF16),
        R3_=v((NARROW, 3, 2, 32, 128), BF16),
        R5_=v((NARROW, 32, 128), BF16),
        w_sem=dma((10,)),
        ar_s=dma((7, 12)),
        ar_r=dma((7, 12)),
        kv_s=dma((2, 2)),
        kv_r=dma((2, 2)),
        pa_s=dma((2, 2)),
        pa_r=dma((2, 2)),
        b_s=dma,
        b_r=dma,
        g0_s=dma((2,)),
        g0_r=dma((2,)),
        rs_s=dma((UNITS + NARROW, 7)),
        rs_r=dma((UNITS + NARROW, 7)),
    )


COLORS = (("y", 0), ("z", 0), ("y", 1), ("z", 1))


class Share:
    def __init__(self, r, here, index, narrow, color, write):
        tail = "_" if narrow else ""
        self.g, self.r1, self.r3, self.r5 = (
            getattr(r, name + tail).at[index] for name in ("G", "R1", "R3", "R5")
        )
        self.narrow = narrow
        self.r2 = None if narrow else r.R2.at[index]
        row = index + (UNITS if narrow else 0)
        self.ss = [r.rs_s.at[row, n] for n in range(7)]
        self.rs = [r.rs_r.at[row, n] for n in range(7)]
        self.here = here
        self.axis, o1 = color
        self.f1, self.f2 = (far, near) if o1 else (near, far)
        self.write = write
        self.stage = 0

    def one(self, value):
        return self.g.at[:, value] if self.axis == "y" else self.g.at[:, :, value]

    def two(self, value):
        if self.axis == "y":
            return self.g.at[:, self.here.y, value]
        return self.g.at[:, value, self.here.z]

    def device(self, first=None, second=None, x=None):
        h = self.here
        y, z = h.y, h.z
        if first is not None:
            y, z = (first, z) if self.axis == "y" else (y, first)
        if second is not None:
            y, z = (y, second) if self.axis == "y" else (second, z)
        x = h.x if x is None else x
        return (x * 16 + y * 4 + z, h.t)

    def send(self, n, source, target, device):
        copy = pltpu.make_async_remote_copy(
            src_ref=source,
            dst_ref=target,
            send_sem=self.ss[n],
            recv_sem=self.rs[n],
            device_id=device,
            device_id_type=MESH,
        )
        copy.start()
        return copy

    def spread(self, n, view, target, to):
        at = (self.here.y, self.here.z)[(self.axis == "z") == (n == 0)]
        copies = []
        for d in range(1, 4):
            peer = lax.rem(at + d, 4)
            copies.append(self.send(n + d - 1, view(peer), target.at[d - 1], to(peer)))
        return copies

    def gather(self, part, others):
        total = part[...].astype(F32)
        for other in others:
            total = total + other[...].astype(F32)
        return total

    def fold(self, part, others):
        part[...] = self.gather(part, others).astype(BF16)

    def advance(self):
        h = self.here
        v, w = (h.y, h.z) if self.axis == "y" else (h.z, h.y)
        stage = self.stage
        if self.narrow and stage:
            stage += 1
        if stage > 4:
            return
        self.stage += 1
        if stage == 0 and self.narrow:
            self.c = self.spread(0, self.one, self.r1, lambda peer: self.device(first=peer))
            return
        if stage == 0:
            peer = self.f1(v)
            to = self.device(first=peer)
            self.c = [
                self.send(0, self.one(peer), self.r1.at[0], to),
                self.send(1, self.one(self.f2(peer)), self.r1.at[1], to),
            ]
            return
        for copy in self.c:
            copy.wait()
        if stage == 1:
            peer = self.f2(v)
            part = self.one(peer)
            self.fold(part, [self.r1.at[1]])
            self.c = [self.send(2, part, self.r2, self.device(first=peer))]
        elif stage == 2:
            if self.narrow:
                self.fold(self.one(v), [self.r1.at[d] for d in range(3)])
            else:
                self.fold(self.one(v), [self.r1.at[0], self.r2])
            self.c = self.spread(3, self.two, self.r3, lambda peer: self.device(second=peer))
        elif stage == 3:
            self.fold(self.two(w), [self.r3.at[d] for d in range(3)])
            other = self.g.at[1 - h.x, h.y, h.z]
            self.c = [self.send(6, other, self.r5, self.device(x=1 - h.x))]
        else:
            self.write(self.gather(self.g.at[h.x, h.y, h.z], [self.r5]))


def norm_vjp(x, gain, dy):
    r = lax.rsqrt(jnp.mean(x * x, axis=-1, keepdims=True) + EPS)
    scaled = dy * gain
    inner = jnp.mean(scaled * x, axis=-1, keepdims=True)
    dx = r * scaled - x * (r * r * r * inner)
    return dx, dy * (x * r)


def kernel(*refs):
    scratches = scratch()
    r = types.SimpleNamespace(**dict(zip(INPUTS + OUTPUTS + tuple(scratches), refs)))
    s = lax.axis_index("seq")
    t = lax.axis_index("tensor")
    here = types.SimpleNamespace(
        x=lax.div(s, 16), y=lax.rem(lax.div(s, 4), 4), z=lax.rem(s, 4), t=t, s=s
    )
    core, chip = lax.rem(t, 2), lax.div(t, 2)
    beside = (s, chip * 2 + 1 - core)
    across = (s, (1 - chip) * 2 + core)
    following = (lax.rem(s + 1, 32), t)
    preceding = (lax.rem(s + 31, 32), t)
    at = lambda x, y, z: (x * 16 + y * 4 + z, t)
    peers = [
        beside,
        across,
        following,
        preceding,
        at(1 - here.x, here.y, here.z),
        at(here.x, near(here.y), here.z),
        at(here.x, far(here.y), here.z),
        at(here.x, here.y, near(here.z)),
        at(here.x, here.y, far(here.z)),
        at(here.x, lax.rem(here.y + 2, 4), here.z),
        at(here.x, here.y, lax.rem(here.z + 2, 4)),
    ]

    loads = {}
    order = [("tok", r.tokens, r.h.at[0])]
    for l in range(LAYERS):
        order.append((("A", l), r.wa.at[l], r.wA.at[l]))
        order.append((("O", l), r.wo.at[l], r.wO.at[l]))
        order.append((("U", l), r.wu.at[l], r.wU.at[l]))
        order.append((("D", l), r.wd.at[l], r.wD.at[l]))
    order.append(("H", r.wh, r.wH))
    for n, (name, source, target) in enumerate(order):
        loads[name] = pltpu.make_async_copy(source, target, r.w_sem.at[n])
        if n < 2:
            loads[name].start()

    barrier = pltpu.get_barrier_semaphore()
    for peer in peers:
        pl.semaphore_signal(barrier, inc=1, device_id=peer, device_id_type=MESH)
    r.gg[...] = jnp.zeros_like(r.gg)
    bound = r.bound[0]
    restart = jnp.where(s == 0, 1, r.reset[0])
    r.bs[...] = jnp.full((8, 256), bound, jnp.int32)

    def remote(source, target, send_sem, recv_sem, device):
        return pltpu.make_async_remote_copy(
            src_ref=source,
            dst_ref=target,
            send_sem=send_sem,
            recv_sem=recv_sem,
            device_id=device,
            device_id_type=MESH,
        )

    def norm_into(source, k, target):
        def rows(i):
            block = span(i, 64)
            x = source[block, :].astype(F32)
            scale = lax.rsqrt(jnp.mean(x * x, axis=-1, keepdims=True) + EPS)
            target[block, :] = (x * scale * r.gains[k : k + 1, :]).astype(BF16)

        loop(4, rows)

    def ar_begin(n, part):
        half, distant = r.ar_half.at[n % 2], r.ar_far.at[n % 2]
        near_copies, far_copies = [], []
        for i in range(4):
            lanes = slice(i * 256, (i + 1) * 256)
            r.ar_send[:, lanes] = part((1 - core) * 128, i).astype(BF16)
            copy = remote(
                r.ar_send.at[:, lanes],
                half.at[:, lanes],
                r.ar_s.at[n, i],
                r.ar_r.at[n, i],
                beside,
            )
            copy.start()
            near_copies.append(copy)
        for i in range(4):
            lanes = slice(i * 256, (i + 1) * 256)
            mine = part(core * 128, i)
            near_copies[i].wait()
            r.ar_sum[:, lanes] = (mine + half[:, lanes].astype(F32)).astype(BF16)
            copy = remote(
                r.ar_sum.at[:, lanes],
                distant.at[:, lanes],
                r.ar_s.at[n, 4 + i],
                r.ar_r.at[n, 4 + i],
                across,
            )
            copy.start()
            far_copies.append(copy)
        return far_copies

    def ar_end(n, far_copies, target, residual):
        mine = pl.ds(pl.multiple_of(core * 128, 128), 128)
        copies = []
        for i in range(4):
            lanes = slice(i * 256, (i + 1) * 256)
            far_copies[i].wait()
            total = r.ar_sum[:, lanes].astype(F32) + r.ar_far[n % 2, :, lanes].astype(F32)
            if residual is not None:
                total = residual[mine, lanes].astype(F32) + total
            target[mine, lanes] = total.astype(BF16)
            copy = remote(
                target.at[mine, lanes],
                target.at[mine, lanes],
                r.ar_s.at[n, 8 + i],
                r.ar_r.at[n, 8 + i],
                beside,
            )
            copy.start()
            copies.append(copy)
        for copy in copies:
            copy.wait()

    def at_rows(base):
        return pl.ds(pl.multiple_of(base, 128), 128)

    loads["tok"].wait()
    own = pl.ds(SEG, SEG)
    for l in range(LAYERS):
        h, a, q, k, v = r.h.at[l], r.a.at[l, own], r.q.at[l], r.k.at[l], r.v.at[l]
        norm_into(h, 2 * l, a)
        loads["A", l].wait()
        if l == 0:
            for name, _, _ in order[2:]:
                loads[name].start()
        k[own, :] = nn(a[...], r.wA[l, 1]).astype(BF16)
        if l == 0:
            pl.semaphore_wait(barrier, len(peers))
            bound_copy = remote(r.bs, r.br, r.b_s, r.b_r, following)
            bound_copy.start()
        send_k = remote(
            k.at[own], k.at[pl.ds(0, SEG)], r.kv_s.at[l, 0], r.kv_r.at[l, 0], following
        )
        send_k.start()
        v[own, :] = nn(a[...], r.wA[l, 2]).astype(BF16)
        send_v = remote(
            v.at[own], v.at[pl.ds(0, SEG)], r.kv_s.at[l, 1], r.kv_r.at[l, 1], following
        )
        send_v.start()
        q[...] = nn(a[...], r.wA[l, 0]).astype(BF16)
        for head in range(2):
            lanes = slice(head * HD, (head + 1) * HD)

            def local(i):
                block = span(i, 128)
                scores = nt(q[block, lanes], k[own, lanes]) * (HD**-0.5)
                row = lax.broadcasted_iota(jnp.int32, (128, SEG), 0) + i * 128
                col = lax.broadcasted_iota(jnp.int32, (128, SEG), 1)
                allowed = (col <= row) & ((col >= bound) | (row < bound))
                r.p[l, head, block, own] = jnp.where(allowed, jnp.exp(scores), 0.0)

            loop(2, local)
        if l == 0:
            bound_copy.wait()
        send_k.wait()
        for head in range(2):
            lanes = slice(head * HD, (head + 1) * HD)

            def memory(i):
                block = span(i, 128)
                scores = nt(q[block, lanes], k[0:SEG, lanes]) * (HD**-0.5)
                row = lax.broadcasted_iota(jnp.int32, (128, SEG), 0) + i * 128
                col = lax.broadcasted_iota(jnp.int32, (128, SEG), 1)
                prior = lax.rem(r.br[0:1, :], SEG)
                allowed = (row < bound) & (restart == 0) & (col >= prior)
                e = jnp.where(allowed, jnp.exp(scores), 0.0)
                e_own = r.p[l, head, block, own]
                total = jnp.sum(e + e_own, axis=-1, keepdims=True)
                r.p[l, head, block, 0:SEG] = e / total
                r.p[l, head, block, own] = e_own / total

            loop(2, memory)
        send_v.wait()
        prev = r.a.at[l, at_rows(core * 128)]
        send_a = remote(
            r.a.at[l, at_rows(SEG + core * 128)],
            prev,
            r.pa_s.at[l, 0],
            r.pa_r.at[l, 0],
            following,
        )
        send_a.start()
        for head in range(2):
            lanes = slice(head * HD, (head + 1) * HD)

            def attend(i):
                block = span(i, 128)
                probs = r.p[l, head, block, :].astype(BF16)
                r.ctx[l, block, lanes] = nn(probs, v[:, lanes]).astype(BF16)

            loop(2, attend)
        loads["O", l].wait()
        copy = ar_begin(
            2 * l, lambda base, i: nt(r.ctx[l, at_rows(base), :], r.wO[l, span(i, 256), :])
        )
        ar_end(2 * l, copy, r.mid.at[l], h)
        norm_into(r.mid.at[l], 2 * l + 1, r.b.at[l])
        loads["U", l].wait()

        def upper(i):
            lanes = span(i, 256)
            u = nn(r.b[l], r.wU[l, :, lanes])
            th = jnp.tanh(ROOT * (u + CUBIC * (u * u * u)))
            half = 0.5 * (1.0 + th)
            r.act[l, :, lanes] = (u * half).astype(BF16)
            r.slope[l, :, lanes] = half + (0.5 * ROOT) * u * (1.0 - th * th) * (
                1.0 + (3.0 * CUBIC) * (u * u)
            )

        loop(4, upper)
        loads["D", l].wait()
        copy = ar_begin(
            2 * l + 1,
            lambda base, i: nt(r.act[l, at_rows(base), :], r.wD[l, span(i, 256), :]),
        )
        send_a.wait()
        share_a = remote(prev, prev, r.pa_s.at[l, 1], r.pa_r.at[l, 1], beside)
        share_a.start()
        ar_end(2 * l + 1, copy, r.h.at[l + 1], r.mid.at[l])
        share_a.wait()

    def transposed(source):
        count = source.shape[0]

        def cols(i):
            lanes = span(i, 256)
            r.xt[lanes, 0:count] = source[:, lanes].T

        loop(4, cols)

    def outer(g, value):
        g[...] = value.astype(BF16).reshape(g.shape)

    def share(index, narrow, color, write):
        return Share(r, here, index, narrow, COLORS[color], write)

    def wide(index, color, left, write):
        unit = share(index, False, color, write)
        outer(unit.g, left())
        unit.advance()
        return unit

    def step(units):
        for unit in units:
            unit.advance()

    def norm_back(source, k, dy_of, add):
        def rows(i):
            block = span(i, 64)
            dx, dg = norm_vjp(source[block, :].astype(F32), r.gains[k : k + 1, :], dy_of(block))
            r.dh[block, :] = (r.dh[block, :] + dx) if add else dx
            r.gg[k] += jnp.sum(dg.reshape(8, 8, D), axis=0)

        loop(4, rows)

    def rounded_dh():
        def rows(i):
            block = span(i, 64)
            r.dy[block, :] = r.dh[block, :].astype(BF16)

        loop(4, rows)

    dq = r.dctx
    loads["H"].wait()
    dq[...] = r.qcot[...].astype(BF16)

    def top(i):
        lanes = span(i, 256)
        r.wide_tmp[:, lanes] = nn(dq[...], r.wH[:, lanes])

    loop(4, top)
    norm_back(r.h.at[2], 4, lambda block: r.wide_tmp[block, :], False)

    def head_grads():
        norm_into(r.h.at[2], 4, r.final)
        r.oe[0:256, :] = nt(r.final[...], r.wH[...])
        transposed(r.final)
        units = []
        for n in range(2):

            def write(value, n=n):
                r.oe[256:288, n * 128 : (n + 1) * 128] = value

            unit = share(n, True, n, write)
            outer(unit.g, nn(r.xt[:, 0:SEG], dq[:, n * 128 : (n + 1) * 128]))
            unit.advance()
            units.append(unit)
        return units

    def ffn_back(l, n):
        rounded_dh()

        def gate(i):
            lanes = span(i, 256)
            d_active = nn(r.dy[...], r.wD[l, :, lanes])
            r.dup[:, lanes] = (d_active * r.slope[l, :, lanes]).astype(BF16)

        loop(4, gate)
        return ar_begin(
            n, lambda base, i: nt(r.dup[at_rows(base), :], r.wU[l, span(i, 256), :])
        )

    def ffn_grads(l):
        units = []
        for kind, (left, right, out) in enumerate(
            ((r.dy, r.act.at[l], 1024), (r.b.at[l], r.dup, 0))
        ):
            transposed(left)
            for n in range(4):

                def write(value, base=out + n * 256):
                    r.oz[l, :, base : base + 256] = value

                units.append(
                    wide(
                        l * 12 + kind * 4 + n,
                        n,
                        lambda n=n, right=right: nn(
                            r.xt[:, 0:SEG], right[:, n * 256 : (n + 1) * 256]
                        ),
                        write,
                    )
                )
        return units

    def attention_back(l):
        norm_back(r.mid.at[l], 2 * l + 1, lambda block: r.db[block, :].astype(F32), True)
        rounded_dh()
        r.dctx[...] = nn(r.dy[...], r.wO[l]).astype(BF16)
        q, k, v = r.q.at[l], r.k.at[l], r.v.at[l]
        for head in range(2):
            lanes = slice(head * HD, (head + 1) * HD)
            d = r.dctx[:, lanes]
            probs = r.p[l, head]
            d_probs = nt(d, v[:, lanes])
            inner = jnp.sum(d_probs * probs, axis=-1, keepdims=True)
            d_scores = (probs * (d_probs - inner) * (HD**-0.5)).astype(BF16)
            r.dqs[:, lanes] = nn(d_scores, k[:, lanes]).astype(BF16)
            r.dkv[0, :, lanes] = tn(d_scores, q[:, lanes]).astype(BF16)
            r.dkv[1, :, lanes] = tn(probs.astype(BF16), d).astype(BF16)

    def unit_index(l, n):
        return l * 12 + 8 + n

    def out_grads(l):
        transposed(r.dy)

        def write(value):
            r.oz[l, :, 2048:2304] = value

        return [wide(unit_index(l, 3), 3, lambda: nn(r.xt[:, 0:SEG], r.ctx[l]), write)]

    def qkv_grads(l):
        transposed(r.a.at[l])
        units = []
        for n in range(3):

            def write(value, base=2304 + n * 256):
                r.oz[l, :, base : base + 256] = value

            def left(n=n):
                if n:
                    return nn(r.xt[...], r.dkv[n - 1])
                return nn(r.xt[:, SEG:], r.dqs[...])

            units.append(wide(unit_index(l, n), n, left, write))
        return units

    def back_part(l):
        def part(base, i):
            total = nt(r.dqs[at_rows(base), :], r.wA[l, 0, span(i, 256), :])
            for n in (1, 2):
                total = total + nt(
                    r.dkv[n - 1, at_rows(SEG + base), :], r.wA[l, n, span(i, 256), :]
                )
            return total

        return part

    copy = ffn_back(1, 4)
    ffn1 = ffn_grads(1)
    heads = head_grads()
    ar_end(4, copy, r.db, None)
    attention_back(1)
    copy = ar_begin(5, back_part(1))
    step(ffn1)
    step(heads)
    attn1 = out_grads(1) + qkv_grads(1)
    ar_end(5, copy, r.db, None)
    norm_back(r.h.at[1], 2, lambda block: r.db[block, :].astype(F32), True)
    copy = ffn_back(0, 6)
    step(ffn1)
    step(heads)
    step(attn1)
    ffn0 = ffn_grads(0)
    ar_end(6, copy, r.db, None)
    attention_back(0)
    attn0 = out_grads(0) + qkv_grads(0)
    step(heads)
    step(ffn1)
    step(attn1)

    def normal(i):
        block = span(i, 64)
        x = r.h[0, block, :].astype(F32)
        r.dh[block, :] = x * lax.rsqrt(jnp.mean(x * x, axis=-1, keepdims=True) + EPS)

    loop(4, normal)
    part = back_part(0)
    for half in range(2):

        def gain(i):
            lanes = span(i, 256)
            rows = pl.ds(half * 128, 128)
            value = part(half * 128, i) * r.dh[rows, lanes]
            r.gg[0, :, lanes] += jnp.sum(value.reshape(16, 8, 256), axis=0)

        loop(4, gain)
    copy = remote(r.gg.at[0], r.g0.at[0], r.g0_s.at[0], r.g0_r.at[0], beside)
    copy.start()
    down0, up0 = ffn0[:4], ffn0[4:]
    step(down0)
    copy.wait()
    r.g0s[...] = r.gg[0] + r.g0[0]
    copy = remote(r.g0s, r.g0.at[1], r.g0_s.at[1], r.g0_r.at[1], across)
    copy.start()
    step(up0)
    copy.wait()
    rows = [jnp.sum(r.g0s[...] + r.g0[1], axis=0, keepdims=True)]
    rows += [jnp.sum(r.gg[n], axis=0, keepdims=True) for n in range(1, 5)]
    table = jnp.concatenate(rows + [jnp.zeros((123, D), F32)], axis=0)

    def write_gains(value):
        r.oe[288:320, 0:128] = value

    unit = share(2, True, 3, write_gains)
    outer(unit.g, table.T)
    unit.advance()
    gain0 = [unit]
    step(ffn1)
    step(attn1)
    step(down0)
    step(attn0)
    step(up0)
    step(gain0)
    step(attn1)
    step(down0)
    step(attn0)
    step(up0)
    step(gain0)
    step(down0)
    step(attn0)
    step(up0)
    step(gain0)
    step(attn0)


def finish(oz, oe, values, attn, out, up, down, head, gains):
    values[...] = oe[0:256, :]
    for n in range(3):
        attn[:, n] = oz[:, :, 2304 + n * 256 : 2560 + n * 256]
    out[...] = oz[:, :, 2048:2304]
    up[...] = oz[:, :, 0:1024]
    down[...] = oz[:, :, 1024:2048]
    head[...] = oe[256:288, :]
    gains[...] = oe[288:320, 0:128].T[0:5, :]


def body(tokens, w_attn, w_out, w_up, w_down, w_head, gains, q_cotangent, bounds, resets):
    vmem = pl.BlockSpec(memory_space=pltpu.VMEM)
    smem = pl.BlockSpec(memory_space=pltpu.SMEM)
    anywhere = pl.BlockSpec(memory_space=pl.ANY)
    shapes = [(2, 32, 3072), (320, 256)]
    outs = pl.pallas_call(
        kernel,
        out_shape=[jax.ShapeDtypeStruct(shape, F32) for shape in shapes],
        in_specs=[anywhere] * 6 + [vmem] * 2 + [smem] * 2,
        out_specs=[vmem] * len(shapes),
        scratch_shapes=list(scratch().values()),
        compiler_params=pltpu.CompilerParams(
            collective_id=0, has_side_effects=True, vmem_limit_bytes=67043328
        ),
    )(
        tokens,
        jnp.transpose(w_attn, (0, 2, 1, 3)),
        w_out,
        w_up,
        w_down,
        w_head,
        gains,
        q_cotangent,
        bounds,
        resets,
    )
    shapes = [
        (256, 256),
        (2, 3, 32, 256),
        (2, 32, 256),
        (2, 32, D),
        (2, 32, D),
        (32, 256),
        (5, 32),
    ]
    values, attn, out, up, down, head, gain = pl.pallas_call(
        finish,
        out_shape=[jax.ShapeDtypeStruct(shape, F32) for shape in shapes],
        in_specs=[vmem] * 2,
        out_specs=[vmem] * len(shapes),
    )(*outs)
    return (values, jnp.transpose(attn, (0, 2, 1, 3)), out, up, down, head.T, gain)


def solution(mesh):
    return jax.shard_map(
        body,
        mesh=mesh,
        in_specs=(
            P("seq", None),
            P(None, None, None, "tensor"),
            P(None, None, "tensor"),
            P(None, None, "tensor"),
            P(None, None, "tensor"),
            P(),
            P(),
            P("seq", None),
            P("seq"),
            P("seq"),
        ),
        out_specs=(
            P("seq", None),
            P(None, "seq", None, "tensor"),
            P(None, "seq", "tensor"),
            P(None, "seq", "tensor"),
            P(None, "seq", "tensor"),
            P(None, "seq"),
            P(None, "seq"),
        ),
        check_vma=False,
    )
```

```python
import functools
import types

import jax
import jax.numpy as jnp
from jax import lax
from jax.experimental import pallas as pl
from jax.experimental.pallas import tpu as pltpu
from jax.sharding import PartitionSpec as P

F32 = jnp.float32
BF16 = jnp.bfloat16
EPS = 1e-06
LAYERS = 2
D = 1024
SEG = 256
HD = 128
CUBIC = 0.044715
ROOT = 0.7978845608028654
MESH = pl.DeviceIdType.MESH
UNITS = 24
NARROW = 2


def nn(a, b):
    return lax.dot_general(a, b, (((1,), (0,)), ((), ())), preferred_element_type=F32)


def nt(a, b):
    return lax.dot_general(a, b, (((1,), (1,)), ((), ())), preferred_element_type=F32)


def tn(a, b):
    return lax.dot_general(a, b, (((0,), (0,)), ((), ())), preferred_element_type=F32)


def loop(count, f):
    def step(i, carry):
        f(i)
        return carry

    lax.fori_loop(0, count, step, 0)


def span(i, size):
    if isinstance(i, int):
        return pl.ds(i * size, size)
    return pl.ds(pl.multiple_of(i * size, size), size)


def near(v):
    return v + 1 - 2 * lax.rem(v, 2)


def far(v):
    return 3 - v


INPUTS = ("tokens", "wa", "wo", "wu", "wd", "wh", "gains", "qcot", "bound", "reset")
OUTPUTS = ("oz", "oe")


def scratch():
    v = pltpu.VMEM
    dma = pltpu.SemaphoreType.DMA
    return dict(
        wA=v((2, 3, D, 256), BF16),
        wO=v((2, D, 256), BF16),
        wU=v((2, D, D), BF16),
        wD=v((2, D, D), BF16),
        wH=v((256, D), BF16),
        h=v((3, SEG, D), BF16),
        a=v((2, 2 * SEG, D), BF16),
        q=v((2, SEG, 256), BF16),
        k=v((2, 2 * SEG, 256), BF16),
        v=v((2, 2 * SEG, 256), BF16),
        p=v((2, 2, SEG, 2 * SEG), F32),
        ctx=v((2, SEG, 256), BF16),
        mid=v((2, SEG, D), BF16),
        b=v((2, SEG, D), BF16),
        slope=v((2, SEG, D), F32),
        act=v((2, SEG, D), BF16),
        ar_send=v((128, D), BF16),
        ar_half=v((2, 128, D), BF16),
        ar_sum=v((128, D), BF16),
        ar_far=v((2, 128, D), BF16),
        db=v((SEG, D), BF16),
        dh=v((SEG, D), F32),
        xt=v((D, 2 * SEG), BF16),
        final=v((SEG, D), BF16),
        dy=v((SEG, D), BF16),
        dup=v((SEG, D), BF16),
        dctx=v((SEG, 256), BF16),
        dqs=v((SEG, 256), BF16),
        dkv=v((2, 2 * SEG, 256), BF16),
        wide_tmp=v((SEG, D), F32),
        gg=v((5, 8, D), F32),
        g0=v((2, 8, D), F32),
        g0s=v((8, D), F32),
        bs=v((8, 256), jnp.int32),
        br=v((8, 256), jnp.int32),
        G=v((UNITS, 2, 4, 4, 32, 256), BF16),
        R1=v((UNITS, 2, 2, 4, 32, 256), BF16),
        R2=v((UNITS, 2, 4, 32, 256), BF16),
        R3=v((UNITS, 3, 2, 32, 256), BF16),
        R5=v((UNITS, 32, 256), BF16),
        G_=v((NARROW, 2, 4, 4, 32, 128), BF16),
        R1_=v((NARROW, 3, 2, 4, 32, 128), BF16),
        R3_=v((NARROW, 3, 2, 32, 128), BF16),
        R5_=v((NARROW, 32, 128), BF16),
        w_sem=dma((10,)),
        ar_s=dma((7, 12)),
        ar_r=dma((7, 12)),
        kv_s=dma((2, 2)),
        kv_r=dma((2, 2)),
        pa_s=dma((2, 2)),
        pa_r=dma((2, 2)),
        hx=v((2, 32, 128), F32),
        hx_s=dma,
        hx_r=dma,
        b_s=dma,
        b_r=dma,
        g0_s=dma((2,)),
        g0_r=dma((2,)),
        rs_s=dma((UNITS + NARROW, 7)),
        rs_r=dma((UNITS + NARROW, 7)),
    )


COLORS = (("y", 0), ("z", 0), ("y", 1), ("z", 1))


class Share:
    def __init__(self, r, here, index, narrow, color, write):
        tail = "_" if narrow else ""
        self.g, self.r1, self.r3, self.r5 = (
            getattr(r, name + tail).at[index] for name in ("G", "R1", "R3", "R5")
        )
        self.narrow = narrow
        self.r2 = None if narrow else r.R2.at[index]
        row = index + (UNITS if narrow else 0)
        self.ss = [r.rs_s.at[row, n] for n in range(7)]
        self.rs = [r.rs_r.at[row, n] for n in range(7)]
        self.here = here
        self.axis, o1 = color
        self.f1, self.f2 = (far, near) if o1 else (near, far)
        self.write = write
        self.stage = 0

    def one(self, value):
        return self.g.at[:, value] if self.axis == "y" else self.g.at[:, :, value]

    def two(self, value):
        if self.axis == "y":
            return self.g.at[:, self.here.y, value]
        return self.g.at[:, value, self.here.z]

    def device(self, first=None, second=None, x=None):
        h = self.here
        y, z = h.y, h.z
        if first is not None:
            y, z = (first, z) if self.axis == "y" else (y, first)
        if second is not None:
            y, z = (y, second) if self.axis == "y" else (second, z)
        x = h.x if x is None else x
        return (x * 16 + y * 4 + z, h.t)

    def send(self, n, source, target, device):
        copy = pltpu.make_async_remote_copy(
            src_ref=source,
            dst_ref=target,
            send_sem=self.ss[n],
            recv_sem=self.rs[n],
            device_id=device,
            device_id_type=MESH,
        )
        copy.start()
        return copy

    def spread(self, n, view, target, to):
        at = (self.here.y, self.here.z)[(self.axis == "z") == (n == 0)]
        copies = []
        for d in range(1, 4):
            peer = lax.rem(at + d, 4)
            copies.append(self.send(n + d - 1, view(peer), target.at[d - 1], to(peer)))
        return copies

    def gather(self, part, others):
        total = part[...].astype(F32)
        for other in others:
            total = total + other[...].astype(F32)
        return total

    def fold(self, part, others):
        part[...] = self.gather(part, others).astype(BF16)

    def advance(self):
        h = self.here
        v, w = (h.y, h.z) if self.axis == "y" else (h.z, h.y)
        stage = self.stage
        if self.narrow and stage:
            stage += 1
        if stage > 4:
            return
        self.stage += 1
        if stage == 0 and self.narrow:
            self.c = self.spread(0, self.one, self.r1, lambda peer: self.device(first=peer))
            return
        if stage == 0:
            peer = self.f1(v)
            to = self.device(first=peer)
            self.c = [
                self.send(0, self.one(peer), self.r1.at[0], to),
                self.send(1, self.one(self.f2(peer)), self.r1.at[1], to),
            ]
            return
        for copy in self.c:
            copy.wait()
        if stage == 1:
            peer = self.f2(v)
            part = self.one(peer)
            self.fold(part, [self.r1.at[1]])
            self.c = [self.send(2, part, self.r2, self.device(first=peer))]
        elif stage == 2:
            if self.narrow:
                self.fold(self.one(v), [self.r1.at[d] for d in range(3)])
            else:
                self.fold(self.one(v), [self.r1.at[0], self.r2])
            self.c = self.spread(3, self.two, self.r3, lambda peer: self.device(second=peer))
        elif stage == 3:
            self.fold(self.two(w), [self.r3.at[d] for d in range(3)])
            other = self.g.at[1 - h.x, h.y, h.z]
            self.c = [self.send(6, other, self.r5, self.device(x=1 - h.x))]
        else:
            self.write(self.gather(self.g.at[h.x, h.y, h.z], [self.r5]))


def norm_vjp(x, gain, dy):
    r = lax.rsqrt(jnp.mean(x * x, axis=-1, keepdims=True) + EPS)
    scaled = dy * gain
    inner = jnp.mean(scaled * x, axis=-1, keepdims=True)
    dx = r * scaled - x * (r * r * r * inner)
    return dx, dy * (x * r)


def kernel(*refs):
    scratches = scratch()
    r = types.SimpleNamespace(**dict(zip(INPUTS + OUTPUTS + tuple(scratches), refs)))
    s = lax.axis_index("seq")
    t = lax.axis_index("tensor")
    here = types.SimpleNamespace(
        x=lax.div(s, 16), y=lax.rem(lax.div(s, 4), 4), z=lax.rem(s, 4), t=t, s=s
    )
    core, chip = lax.rem(t, 2), lax.div(t, 2)
    beside = (s, chip * 2 + 1 - core)
    across = (s, (1 - chip) * 2 + core)
    following = (lax.rem(s + 1, 32), t)
    preceding = (lax.rem(s + 31, 32), t)
    at = lambda x, y, z: (x * 16 + y * 4 + z, t)
    peers = [
        beside,
        across,
        following,
        preceding,
        at(1 - here.x, here.y, here.z),
        at(here.x, near(here.y), here.z),
        at(here.x, far(here.y), here.z),
        at(here.x, here.y, near(here.z)),
        at(here.x, here.y, far(here.z)),
        at(here.x, lax.rem(here.y + 2, 4), here.z),
        at(here.x, here.y, lax.rem(here.z + 2, 4)),
    ]

    loads = {}
    order = [("tok", r.tokens, r.h.at[0])]
    for l in range(LAYERS):
        order.append((("A", l), r.wa.at[l], r.wA.at[l]))
        order.append((("O", l), r.wo.at[l], r.wO.at[l]))
        order.append((("U", l), r.wu.at[l], r.wU.at[l]))
        order.append((("D", l), r.wd.at[l], r.wD.at[l]))
    order.append(("H", r.wh, r.wH))
    for n, (name, source, target) in enumerate(order):
        loads[name] = pltpu.make_async_copy(source, target, r.w_sem.at[n])
        if n < 2:
            loads[name].start()

    barrier = pltpu.get_barrier_semaphore()
    for peer in peers:
        pl.semaphore_signal(barrier, inc=1, device_id=peer, device_id_type=MESH)
    r.gg[...] = jnp.zeros_like(r.gg)
    bound = r.bound[0]
    restart = jnp.where(s == 0, 1, r.reset[0])
    r.bs[...] = jnp.full((8, 256), bound, jnp.int32)

    def remote(source, target, send_sem, recv_sem, device):
        return pltpu.make_async_remote_copy(
            src_ref=source,
            dst_ref=target,
            send_sem=send_sem,
            recv_sem=recv_sem,
            device_id=device,
            device_id_type=MESH,
        )

    def norm_into(source, k, target):
        def rows(i):
            block = span(i, 64)
            x = source[block, :].astype(F32)
            scale = lax.rsqrt(jnp.mean(x * x, axis=-1, keepdims=True) + EPS)
            target[block, :] = (x * scale * r.gains[k : k + 1, :]).astype(BF16)

        loop(4, rows)

    def ar_begin(n, part):
        half, distant = r.ar_half.at[n % 2], r.ar_far.at[n % 2]
        near_copies, far_copies, own_parts = [], [], []

        def give(i):
            lanes = slice(i * 256, (i + 1) * 256)
            r.ar_send[:, lanes] = part((1 - core) * 128, i).astype(BF16)
            copy = remote(
                r.ar_send.at[:, lanes],
                half.at[:, lanes],
                r.ar_s.at[n, i],
                r.ar_r.at[n, i],
                beside,
            )
            copy.start()
            near_copies.append(copy)

        def keep(i):
            own_parts.append(part(core * 128, i))

        def pass_on(i):
            lanes = slice(i * 256, (i + 1) * 256)
            near_copies[i].wait()
            r.ar_sum[:, lanes] = (own_parts[i] + half[:, lanes].astype(F32)).astype(BF16)
            copy = remote(
                r.ar_sum.at[:, lanes],
                distant.at[:, lanes],
                r.ar_s.at[n, 4 + i],
                r.ar_r.at[n, 4 + i],
                across,
            )
            copy.start()
            far_copies.append(copy)

        give(0)
        give(1)
        keep(0)
        give(2)
        pass_on(0)
        keep(1)
        give(3)
        pass_on(1)
        keep(2)
        pass_on(2)
        keep(3)
        pass_on(3)
        return far_copies

    def ar_end(n, far_copies, target, residual):
        mine = pl.ds(pl.multiple_of(core * 128, 128), 128)
        copies = []
        for i in range(4):
            lanes = slice(i * 256, (i + 1) * 256)
            far_copies[i].wait()
            total = r.ar_sum[:, lanes].astype(F32) + r.ar_far[n % 2, :, lanes].astype(F32)
            if residual is not None:
                total = residual[mine, lanes].astype(F32) + total
            target[mine, lanes] = total.astype(BF16)
            copy = remote(
                target.at[mine, lanes],
                target.at[mine, lanes],
                r.ar_s.at[n, 8 + i],
                r.ar_r.at[n, 8 + i],
                beside,
            )
            copy.start()
            copies.append(copy)
        for copy in copies:
            copy.wait()

    def at_rows(base):
        return pl.ds(pl.multiple_of(base, 128), 128)

    loads["tok"].wait()
    own = pl.ds(SEG, SEG)
    for l in range(LAYERS):
        h, a, q, k, v = r.h.at[l], r.a.at[l, own], r.q.at[l], r.k.at[l], r.v.at[l]
        norm_into(h, 2 * l, a)
        loads["A", l].wait()
        if l == 0:
            for name, _, _ in order[2:]:
                loads[name].start()
        k[own, :] = nn(a[...], r.wA[l, 1]).astype(BF16)
        if l == 0:
            pl.semaphore_wait(barrier, len(peers))
            bound_copy = remote(r.bs, r.br, r.b_s, r.b_r, following)
            bound_copy.start()
        send_k = remote(
            k.at[own], k.at[pl.ds(0, SEG)], r.kv_s.at[l, 0], r.kv_r.at[l, 0], following
        )
        send_k.start()
        v[own, :] = nn(a[...], r.wA[l, 2]).astype(BF16)
        send_v = remote(
            v.at[own], v.at[pl.ds(0, SEG)], r.kv_s.at[l, 1], r.kv_r.at[l, 1], following
        )
        send_v.start()
        q[...] = nn(a[...], r.wA[l, 0]).astype(BF16)
        for head in range(2):
            lanes = slice(head * HD, (head + 1) * HD)

            def local(i):
                block = span(i, 128)
                scores = nt(q[block, lanes], k[own, lanes]) * (HD**-0.5)
                row = lax.broadcasted_iota(jnp.int32, (128, SEG), 0) + i * 128
                col = lax.broadcasted_iota(jnp.int32, (128, SEG), 1)
                allowed = (col <= row) & ((col >= bound) | (row < bound))
                r.p[l, head, block, own] = jnp.where(allowed, jnp.exp(scores), 0.0)

            loop(2, local)
        if l == 0:
            bound_copy.wait()
        send_k.wait()
        for head in range(2):
            lanes = slice(head * HD, (head + 1) * HD)

            def memory(i):
                block = span(i, 128)
                scores = nt(q[block, lanes], k[0:SEG, lanes]) * (HD**-0.5)
                row = lax.broadcasted_iota(jnp.int32, (128, SEG), 0) + i * 128
                col = lax.broadcasted_iota(jnp.int32, (128, SEG), 1)
                prior = lax.rem(r.br[0:1, :], SEG)
                allowed = (row < bound) & (restart == 0) & (col >= prior)
                e = jnp.where(allowed, jnp.exp(scores), 0.0)
                e_own = r.p[l, head, block, own]
                total = jnp.sum(e + e_own, axis=-1, keepdims=True)
                r.p[l, head, block, 0:SEG] = e / total
                r.p[l, head, block, own] = e_own / total

            loop(2, memory)
        send_v.wait()
        prev = r.a.at[l, at_rows(core * 128)]
        send_a = remote(
            r.a.at[l, at_rows(SEG + core * 128)],
            prev,
            r.pa_s.at[l, 0],
            r.pa_r.at[l, 0],
            following,
        )
        send_a.start()
        for head in range(2):
            lanes = slice(head * HD, (head + 1) * HD)

            def attend(i):
                block = span(i, 128)
                probs = r.p[l, head, block, :].astype(BF16)
                r.ctx[l, block, lanes] = nn(probs, v[:, lanes]).astype(BF16)

            loop(2, attend)
        loads["O", l].wait()
        copy = ar_begin(
            2 * l, lambda base, i: nt(r.ctx[l, at_rows(base), :], r.wO[l, span(i, 256), :])
        )
        ar_end(2 * l, copy, r.mid.at[l], h)
        norm_into(r.mid.at[l], 2 * l + 1, r.b.at[l])
        loads["U", l].wait()

        def upper(i):
            lanes = span(i, 256)
            u = nn(r.b[l], r.wU[l, :, lanes])
            th = jnp.tanh(ROOT * (u + CUBIC * (u * u * u)))
            half = 0.5 * (1.0 + th)
            r.act[l, :, lanes] = (u * half).astype(BF16)
            r.slope[l, :, lanes] = half + (0.5 * ROOT) * u * (1.0 - th * th) * (
                1.0 + (3.0 * CUBIC) * (u * u)
            )

        loop(4, upper)
        loads["D", l].wait()
        copy = ar_begin(
            2 * l + 1,
            lambda base, i: nt(r.act[l, at_rows(base), :], r.wD[l, span(i, 256), :]),
        )
        send_a.wait()
        share_a = remote(prev, prev, r.pa_s.at[l, 1], r.pa_r.at[l, 1], beside)
        share_a.start()
        ar_end(2 * l + 1, copy, r.h.at[l + 1], r.mid.at[l])
        share_a.wait()

    def transposed(source):
        count = source.shape[0]

        def cols(i):
            lanes = span(i, 256)
            r.xt[lanes, 0:count] = source[:, lanes].T

        loop(4, cols)

    def outer(g, value):
        g[...] = value.astype(BF16).reshape(g.shape)

    def share(index, narrow, color, write):
        return Share(r, here, index, narrow, COLORS[color], write)

    def wide(index, color, left, write):
        unit = share(index, False, color, write)
        outer(unit.g, left())
        unit.advance()
        return unit

    def step(units):
        for unit in units:
            unit.advance()

    def norm_back(source, k, dy_of, add):
        def rows(i):
            block = span(i, 64)
            dx, dg = norm_vjp(source[block, :].astype(F32), r.gains[k : k + 1, :], dy_of(block))
            r.dh[block, :] = (r.dh[block, :] + dx) if add else dx
            r.gg[k] += jnp.sum(dg.reshape(8, 8, D), axis=0)

        loop(4, rows)

    def rounded_dh():
        def rows(i):
            block = span(i, 64)
            r.dy[block, :] = r.dh[block, :].astype(BF16)

        loop(4, rows)

    dq = r.dctx
    loads["H"].wait()
    dq[...] = r.qcot[...].astype(BF16)

    def top(i):
        lanes = span(i, 256)
        r.wide_tmp[:, lanes] = nn(dq[...], r.wH[:, lanes])

    loop(4, top)
    norm_back(r.h.at[2], 4, lambda block: r.wide_tmp[block, :], False)

    def head_grads():
        norm_into(r.h.at[2], 4, r.final)
        r.oe[0:256, :] = nt(r.final[...], r.wH[...])
        transposed(r.final)
        r.hx_copy = remote(r.hx.at[0], r.hx.at[1], r.hx_s, r.hx_r, beside)

        def write(value):
            r.hx[0] = value
            r.hx_copy.start()

        unit = share(0, True, 0, write)
        outer(unit.g, nn(r.xt[:, 0:SEG], dq[:, span(core, 128)]))
        unit.advance()
        return [unit]

    def head_done():
        r.hx_copy.wait()
        r.oe[256:288, span(core, 128)] = r.hx[0]
        r.oe[256:288, span(1 - core, 128)] = r.hx[1]

    def ffn_back(l, n, early=False):
        rounded_dh()
        down = ffn_kind(l, 0) if early else []

        def gate(i):
            lanes = span(i, 256)
            d_active = nn(r.dy[...], r.wD[l, :, lanes])
            r.dup[:, lanes] = (d_active * r.slope[l, :, lanes]).astype(BF16)

        loop(4, gate)
        return down, ar_begin(
            n, lambda base, i: nt(r.dup[at_rows(base), :], r.wU[l, span(i, 256), :])
        )

    def ffn_kind(l, kind):
        left, right, out = ((r.dy, r.act.at[l], 1024), (r.b.at[l], r.dup, 0))[kind]
        transposed(left)
        units = []
        for n in range(4):

            def write(value, base=out + n * 256):
                r.oz[l, :, base : base + 256] = value

            def block(n=n):
                return nn(r.xt[:, 0:SEG], right[:, n * 256 : (n + 1) * 256])

            units.append(wide(l * 12 + kind * 4 + n, n, block, write))
        return units

    def attention_back(l):
        norm_back(r.mid.at[l], 2 * l + 1, lambda block: r.db[block, :].astype(F32), True)
        rounded_dh()
        r.dctx[...] = nn(r.dy[...], r.wO[l]).astype(BF16)
        q, k, v = r.q.at[l], r.k.at[l], r.v.at[l]
        for head in range(2):
            lanes = slice(head * HD, (head + 1) * HD)
            d = r.dctx[:, lanes]
            probs = r.p[l, head]
            d_probs = nt(d, v[:, lanes])
            inner = jnp.sum(d_probs * probs, axis=-1, keepdims=True)
            d_scores = (probs * (d_probs - inner) * (HD**-0.5)).astype(BF16)
            r.dqs[:, lanes] = nn(d_scores, k[:, lanes]).astype(BF16)
            r.dkv[0, :, lanes] = tn(d_scores, q[:, lanes]).astype(BF16)
            r.dkv[1, :, lanes] = tn(probs.astype(BF16), d).astype(BF16)

    def unit_index(l, n):
        return l * 12 + 8 + n

    def out_grads(l):
        transposed(r.dy)

        def write(value):
            r.oz[l, :, 2048:2304] = value

        return [wide(unit_index(l, 3), 3, lambda: nn(r.xt[:, 0:SEG], r.ctx[l]), write)]

    def qkv_grads(l):
        transposed(r.a.at[l])
        units = []
        for n in range(3):

            def write(value, base=2304 + n * 256):
                r.oz[l, :, base : base + 256] = value

            def left(n=n):
                if n:
                    return nn(r.xt[...], r.dkv[n - 1])
                return nn(r.xt[:, SEG:], r.dqs[...])

            units.append(wide(unit_index(l, n), n, left, write))
        return units

    def back_part(l):
        def part(base, i):
            total = nt(r.dqs[at_rows(base), :], r.wA[l, 0, span(i, 256), :])
            for n in (1, 2):
                total = total + nt(
                    r.dkv[n - 1, at_rows(SEG + base), :], r.wA[l, n, span(i, 256), :]
                )
            return total

        return part

    down1, copy = ffn_back(1, 4, True)
    up1 = ffn_kind(1, 1)
    heads = head_grads()
    step(down1)
    ar_end(4, copy, r.db, None)
    attention_back(1)
    copy = ar_begin(5, back_part(1))
    attn1 = out_grads(1) + qkv_grads(1)
    step(up1)
    step(down1)
    step(heads)
    ar_end(5, copy, r.db, None)
    norm_back(r.h.at[1], 2, lambda block: r.db[block, :].astype(F32), True)
    _, copy = ffn_back(0, 6)
    down0 = ffn_kind(0, 0)
    up0 = ffn_kind(0, 1)
    step(up1)
    step(attn1)
    step(heads)
    ar_end(6, copy, r.db, None)
    attention_back(0)
    attn0 = out_grads(0) + qkv_grads(0)
    step(down1)
    step(heads)

    def normal(i):
        block = span(i, 64)
        x = r.h[0, block, :].astype(F32)
        r.dh[block, :] = x * lax.rsqrt(jnp.mean(x * x, axis=-1, keepdims=True) + EPS)

    loop(4, normal)
    part = back_part(0)
    for half in range(2):

        def gain(i):
            lanes = span(i, 256)
            rows = pl.ds(half * 128, 128)
            value = part(half * 128, i) * r.dh[rows, lanes]
            r.gg[0, :, lanes] += jnp.sum(value.reshape(16, 8, 256), axis=0)

        loop(4, gain)
    copy = remote(r.gg.at[0], r.g0.at[0], r.g0_s.at[0], r.g0_r.at[0], beside)
    copy.start()
    step(down0)
    copy.wait()
    r.g0s[...] = r.gg[0] + r.g0[0]
    copy = remote(r.g0s, r.g0.at[1], r.g0_s.at[1], r.g0_r.at[1], across)
    copy.start()
    step(attn1)
    step(up1)
    step(up0)
    copy.wait()
    rows = [jnp.sum(r.g0s[...] + r.g0[1], axis=0, keepdims=True)]
    rows += [jnp.sum(r.gg[n], axis=0, keepdims=True) for n in range(1, 5)]
    table = jnp.concatenate(rows + [jnp.zeros((123, D), F32)], axis=0)

    def write_gains(value):
        r.oe[288:320, 0:128] = value

    unit = share(1, True, 3, write_gains)
    outer(unit.g, table.T)
    unit.advance()
    gain0 = [unit]
    step(down1)
    step(down0)
    step(attn0)
    step(up1)
    step(attn1)
    step(up0)
    step(gain0)
    step(down0)
    step(attn0)
    step(attn1)
    step(up0)
    step(gain0)
    step(down0)
    step(attn0)
    step(up0)
    step(gain0)
    head_done()
    step(attn0)


def finish(oz, oe, values, attn, out, up, down, head, gains):
    values[...] = oe[0:256, :]
    for n in range(3):
        attn[:, n] = oz[:, :, 2304 + n * 256 : 2560 + n * 256]
    out[...] = oz[:, :, 2048:2304]
    up[...] = oz[:, :, 0:1024]
    down[...] = oz[:, :, 1024:2048]
    head[...] = oe[256:288, :]
    gains[...] = oe[288:320, 0:128].T[0:5, :]


def body(tokens, w_attn, w_out, w_up, w_down, w_head, gains, q_cotangent, bounds, resets):
    vmem = pl.BlockSpec(memory_space=pltpu.VMEM)
    smem = pl.BlockSpec(memory_space=pltpu.SMEM)
    anywhere = pl.BlockSpec(memory_space=pl.ANY)
    shapes = [(2, 32, 3072), (320, 256)]
    outs = pl.pallas_call(
        kernel,
        out_shape=[jax.ShapeDtypeStruct(shape, F32) for shape in shapes],
        in_specs=[anywhere] * 6 + [vmem] * 2 + [smem] * 2,
        out_specs=[vmem] * len(shapes),
        scratch_shapes=list(scratch().values()),
        compiler_params=pltpu.CompilerParams(
            collective_id=0, has_side_effects=True, vmem_limit_bytes=67043328
        ),
    )(
        tokens,
        jnp.transpose(w_attn, (0, 2, 1, 3)),
        w_out,
        w_up,
        w_down,
        w_head,
        gains,
        q_cotangent,
        bounds,
        resets,
    )
    shapes = [
        (256, 256),
        (2, 3, 32, 256),
        (2, 32, 256),
        (2, 32, D),
        (2, 32, D),
        (32, 256),
        (5, 32),
    ]
    values, attn, out, up, down, head, gain = pl.pallas_call(
        finish,
        out_shape=[jax.ShapeDtypeStruct(shape, F32) for shape in shapes],
        in_specs=[vmem] * 2,
        out_specs=[vmem] * len(shapes),
    )(*outs)
    return (values, jnp.transpose(attn, (0, 2, 1, 3)), out, up, down, head.T, gain)


def solution(mesh):
    return jax.shard_map(
        body,
        mesh=mesh,
        in_specs=(
            P("seq", None),
            P(None, None, None, "tensor"),
            P(None, None, "tensor"),
            P(None, None, "tensor"),
            P(None, None, "tensor"),
            P(),
            P(),
            P("seq", None),
            P("seq"),
            P("seq"),
        ),
        out_specs=(
            P("seq", None),
            P(None, "seq", None, "tensor"),
            P(None, "seq", "tensor"),
            P(None, "seq", "tensor"),
            P(None, "seq", "tensor"),
            P(None, "seq"),
            P(None, "seq"),
        ),
        check_vma=False,
    )
```

```python
import functools
import types

import jax
import jax.numpy as jnp
from jax import lax
from jax.experimental import pallas as pl
from jax.experimental.pallas import tpu as pltpu
from jax.sharding import PartitionSpec as P

F32 = jnp.float32
BF16 = jnp.bfloat16
EPS = 1e-06
LAYERS = 2
D = 1024
SEG = 256
HD = 128
CUBIC = 0.044715
ROOT = 0.7978845608028654
MESH = pl.DeviceIdType.MESH
UNITS = 24
NARROW = 2


def nn(a, b):
    return lax.dot_general(a, b, (((1,), (0,)), ((), ())), preferred_element_type=F32)


def nt(a, b):
    return lax.dot_general(a, b, (((1,), (1,)), ((), ())), preferred_element_type=F32)


def tn(a, b):
    return lax.dot_general(a, b, (((0,), (0,)), ((), ())), preferred_element_type=F32)


def loop(count, f):
    def step(i, carry):
        f(i)
        return carry

    lax.fori_loop(0, count, step, 0)


def span(i, size):
    if isinstance(i, int):
        return pl.ds(i * size, size)
    return pl.ds(pl.multiple_of(i * size, size), size)


def near(v):
    return v + 1 - 2 * lax.rem(v, 2)


def far(v):
    return 3 - v


INPUTS = ("tokens", "wa", "wo", "wu", "wd", "wh", "gains", "qcot", "bound", "reset")
OUTPUTS = ("oz", "oe")


def scratch():
    v = pltpu.VMEM
    dma = pltpu.SemaphoreType.DMA
    return dict(
        wA=v((2, 3, D, 256), BF16),
        wO=v((2, D, 256), BF16),
        wU=v((2, D, D), BF16),
        wD=v((2, D, D), BF16),
        wH=v((256, D), BF16),
        h=v((3, SEG, D), BF16),
        a=v((2, 2 * SEG, D), BF16),
        q=v((2, SEG, 256), BF16),
        k=v((2, 2 * SEG, 256), BF16),
        v=v((2, 2 * SEG, 256), BF16),
        p=v((2, 2, SEG, 2 * SEG), F32),
        ctx=v((2, SEG, 256), BF16),
        mid=v((2, SEG, D), BF16),
        b=v((2, SEG, D), BF16),
        slope=v((2, SEG, D), F32),
        act=v((2, SEG, D), BF16),
        ar_send=v((128, D), BF16),
        ar_half=v((2, 128, D), BF16),
        ar_sum=v((128, D), BF16),
        ar_far=v((2, 128, D), BF16),
        db=v((SEG, D), BF16),
        dh=v((SEG, D), F32),
        xt=v((D, 2 * SEG), BF16),
        final=v((SEG, D), BF16),
        dy=v((SEG, D), BF16),
        dup=v((SEG, D), BF16),
        dctx=v((SEG, 256), BF16),
        dqs=v((SEG, 256), BF16),
        dkv=v((2, 2 * SEG, 256), BF16),
        wide_tmp=v((SEG, D), F32),
        gg=v((5, 8, D), F32),
        g0=v((2, 8, D), F32),
        g0s=v((8, D), F32),
        bs=v((8, 256), jnp.int32),
        br=v((8, 256), jnp.int32),
        G=v((UNITS, 2, 4, 4, 32, 256), BF16),
        R1=v((UNITS, 2, 2, 4, 32, 256), BF16),
        R2=v((UNITS, 2, 4, 32, 256), BF16),
        R3=v((UNITS, 3, 2, 32, 256), BF16),
        R5=v((UNITS, 32, 256), BF16),
        G_=v((NARROW, 2, 4, 4, 32, 128), BF16),
        R1_=v((NARROW, 3, 2, 4, 32, 128), BF16),
        R3_=v((NARROW, 3, 2, 32, 128), BF16),
        R5_=v((NARROW, 32, 128), BF16),
        w_sem=dma((10,)),
        ar_s=dma((7, 12)),
        ar_r=dma((7, 12)),
        kv_s=dma((2, 2)),
        kv_r=dma((2, 2)),
        pa_s=dma((2, 2)),
        pa_r=dma((2, 2)),
        hx=v((2, 32, 128), F32),
        hx_s=dma,
        hx_r=dma,
        b_s=dma,
        b_r=dma,
        g0_s=dma((2,)),
        g0_r=dma((2,)),
        rs_s=dma((UNITS + NARROW, 7)),
        rs_r=dma((UNITS + NARROW, 7)),
    )


COLORS = (("y", 0), ("z", 0), ("y", 1), ("z", 1))


class Share:
    def __init__(self, r, here, index, narrow, color, write):
        tail = "_" if narrow else ""
        self.g, self.r1, self.r3, self.r5 = (
            getattr(r, name + tail).at[index] for name in ("G", "R1", "R3", "R5")
        )
        self.narrow = narrow
        self.r2 = None if narrow else r.R2.at[index]
        row = index + (UNITS if narrow else 0)
        self.ss = [r.rs_s.at[row, n] for n in range(7)]
        self.rs = [r.rs_r.at[row, n] for n in range(7)]
        self.here = here
        self.axis, o1 = color
        self.f1, self.f2 = (far, near) if o1 else (near, far)
        self.write = write
        self.stage = 0

    def one(self, value):
        return self.g.at[:, value] if self.axis == "y" else self.g.at[:, :, value]

    def two(self, value):
        if self.axis == "y":
            return self.g.at[:, self.here.y, value]
        return self.g.at[:, value, self.here.z]

    def device(self, first=None, second=None, x=None):
        h = self.here
        y, z = h.y, h.z
        if first is not None:
            y, z = (first, z) if self.axis == "y" else (y, first)
        if second is not None:
            y, z = (y, second) if self.axis == "y" else (second, z)
        x = h.x if x is None else x
        return (x * 16 + y * 4 + z, h.t)

    def send(self, n, source, target, device):
        copy = pltpu.make_async_remote_copy(
            src_ref=source,
            dst_ref=target,
            send_sem=self.ss[n],
            recv_sem=self.rs[n],
            device_id=device,
            device_id_type=MESH,
        )
        copy.start()
        return copy

    def spread(self, n, view, target, to):
        at = (self.here.y, self.here.z)[(self.axis == "z") == (n == 0)]
        copies = []
        for d in range(1, 4):
            peer = lax.rem(at + d, 4)
            copies.append(self.send(n + d - 1, view(peer), target.at[d - 1], to(peer)))
        return copies

    def gather(self, part, others):
        total = part[...].astype(F32)
        for other in others:
            total = total + other[...].astype(F32)
        return total

    def fold(self, part, others):
        part[...] = self.gather(part, others).astype(BF16)

    def advance(self):
        h = self.here
        v, w = (h.y, h.z) if self.axis == "y" else (h.z, h.y)
        stage = self.stage
        if self.narrow and stage:
            stage += 1
        if stage > 4:
            return
        self.stage += 1
        if stage == 0 and self.narrow:
            self.c = self.spread(0, self.one, self.r1, lambda peer: self.device(first=peer))
            return
        if stage == 0:
            peer = self.f1(v)
            to = self.device(first=peer)
            self.c = [
                self.send(0, self.one(peer), self.r1.at[0], to),
                self.send(1, self.one(self.f2(peer)), self.r1.at[1], to),
            ]
            return
        for copy in self.c:
            copy.wait()
        if stage == 1:
            peer = self.f2(v)
            part = self.one(peer)
            self.fold(part, [self.r1.at[1]])
            self.c = [self.send(2, part, self.r2, self.device(first=peer))]
        elif stage == 2:
            if self.narrow:
                self.fold(self.one(v), [self.r1.at[d] for d in range(3)])
            else:
                self.fold(self.one(v), [self.r1.at[0], self.r2])
            self.c = self.spread(3, self.two, self.r3, lambda peer: self.device(second=peer))
        elif stage == 3:
            self.fold(self.two(w), [self.r3.at[d] for d in range(3)])
            other = self.g.at[1 - h.x, h.y, h.z]
            self.c = [self.send(6, other, self.r5, self.device(x=1 - h.x))]
        else:
            self.write(self.gather(self.g.at[h.x, h.y, h.z], [self.r5]))


def norm_vjp(x, gain, dy):
    r = lax.rsqrt(jnp.mean(x * x, axis=-1, keepdims=True) + EPS)
    scaled = dy * gain
    inner = jnp.mean(scaled * x, axis=-1, keepdims=True)
    dx = r * scaled - x * (r * r * r * inner)
    return dx, dy * (x * r)


def kernel(*refs):
    scratches = scratch()
    r = types.SimpleNamespace(**dict(zip(INPUTS + OUTPUTS + tuple(scratches), refs)))
    s = lax.axis_index("seq")
    t = lax.axis_index("tensor")
    here = types.SimpleNamespace(
        x=lax.div(s, 16), y=lax.rem(lax.div(s, 4), 4), z=lax.rem(s, 4), t=t, s=s
    )
    core, chip = lax.rem(t, 2), lax.div(t, 2)
    beside = (s, chip * 2 + 1 - core)
    across = (s, (1 - chip) * 2 + core)
    following = (lax.rem(s + 1, 32), t)
    preceding = (lax.rem(s + 31, 32), t)
    at = lambda x, y, z: (x * 16 + y * 4 + z, t)
    peers = [
        beside,
        across,
        following,
        preceding,
        at(1 - here.x, here.y, here.z),
        at(here.x, near(here.y), here.z),
        at(here.x, far(here.y), here.z),
        at(here.x, here.y, near(here.z)),
        at(here.x, here.y, far(here.z)),
        at(here.x, lax.rem(here.y + 2, 4), here.z),
        at(here.x, here.y, lax.rem(here.z + 2, 4)),
    ]

    loads = {}
    order = [("tok", r.tokens, r.h.at[0])]
    for l in range(LAYERS):
        order.append((("A", l), r.wa.at[l], r.wA.at[l]))
        order.append((("O", l), r.wo.at[l], r.wO.at[l]))
        order.append((("U", l), r.wu.at[l], r.wU.at[l]))
        order.append((("D", l), r.wd.at[l], r.wD.at[l]))
    order.append(("H", r.wh, r.wH))
    for n, (name, source, target) in enumerate(order):
        loads[name] = pltpu.make_async_copy(source, target, r.w_sem.at[n])
        if n < 2:
            loads[name].start()

    barrier = pltpu.get_barrier_semaphore()
    for peer in peers:
        pl.semaphore_signal(barrier, inc=1, device_id=peer, device_id_type=MESH)
    r.gg[...] = jnp.zeros_like(r.gg)
    bound = r.bound[0]
    restart = jnp.where(s == 0, 1, r.reset[0])
    r.bs[...] = jnp.full((8, 256), bound, jnp.int32)

    def remote(source, target, send_sem, recv_sem, device):
        return pltpu.make_async_remote_copy(
            src_ref=source,
            dst_ref=target,
            send_sem=send_sem,
            recv_sem=recv_sem,
            device_id=device,
            device_id_type=MESH,
        )

    def norm_into(source, k, target):
        def rows(i):
            block = span(i, 64)
            x = source[block, :].astype(F32)
            scale = lax.rsqrt(jnp.mean(x * x, axis=-1, keepdims=True) + EPS)
            target[block, :] = (x * scale * r.gains[k : k + 1, :]).astype(BF16)

        loop(4, rows)

    def ar_begin(n, part):
        half, distant = r.ar_half.at[n % 2], r.ar_far.at[n % 2]
        near_copies, far_copies, own_parts = [], [], []

        def give(i):
            lanes = slice(i * 256, (i + 1) * 256)
            r.ar_send[:, lanes] = part((1 - core) * 128, i).astype(BF16)
            copy = remote(
                r.ar_send.at[:, lanes],
                half.at[:, lanes],
                r.ar_s.at[n, i],
                r.ar_r.at[n, i],
                beside,
            )
            copy.start()
            near_copies.append(copy)

        def keep(i):
            own_parts.append(part(core * 128, i))

        def pass_on(i):
            lanes = slice(i * 256, (i + 1) * 256)
            near_copies[i].wait()
            r.ar_sum[:, lanes] = (own_parts[i] + half[:, lanes].astype(F32)).astype(BF16)
            copy = remote(
                r.ar_sum.at[:, lanes],
                distant.at[:, lanes],
                r.ar_s.at[n, 4 + i],
                r.ar_r.at[n, 4 + i],
                across,
            )
            copy.start()
            far_copies.append(copy)

        give(0)
        give(1)
        keep(0)
        give(2)
        pass_on(0)
        keep(1)
        give(3)
        pass_on(1)
        keep(2)
        pass_on(2)
        keep(3)
        pass_on(3)
        return far_copies

    def ar_end(n, far_copies, target, residual):
        mine = pl.ds(pl.multiple_of(core * 128, 128), 128)
        copies = []
        for i in range(4):
            lanes = slice(i * 256, (i + 1) * 256)
            far_copies[i].wait()
            total = r.ar_sum[:, lanes].astype(F32) + r.ar_far[n % 2, :, lanes].astype(F32)
            if residual is not None:
                total = residual[mine, lanes].astype(F32) + total
            target[mine, lanes] = total.astype(BF16)
            copy = remote(
                target.at[mine, lanes],
                target.at[mine, lanes],
                r.ar_s.at[n, 8 + i],
                r.ar_r.at[n, 8 + i],
                beside,
            )
            copy.start()
            copies.append(copy)
        for copy in copies:
            copy.wait()

    def at_rows(base):
        return pl.ds(pl.multiple_of(base, 128), 128)

    loads["tok"].wait()
    own = pl.ds(SEG, SEG)
    for l in range(LAYERS):
        h, a, q, k, v = r.h.at[l], r.a.at[l, own], r.q.at[l], r.k.at[l], r.v.at[l]
        norm_into(h, 2 * l, a)
        loads["A", l].wait()
        if l == 0:
            for name, _, _ in order[2:]:
                loads[name].start()
        k[own, :] = nn(a[...], r.wA[l, 1]).astype(BF16)
        if l == 0:
            pl.semaphore_wait(barrier, len(peers))
            bound_copy = remote(r.bs, r.br, r.b_s, r.b_r, following)
            bound_copy.start()
        send_k = remote(
            k.at[own], k.at[pl.ds(0, SEG)], r.kv_s.at[l, 0], r.kv_r.at[l, 0], following
        )
        send_k.start()
        v[own, :] = nn(a[...], r.wA[l, 2]).astype(BF16)
        send_v = remote(
            v.at[own], v.at[pl.ds(0, SEG)], r.kv_s.at[l, 1], r.kv_r.at[l, 1], following
        )
        send_v.start()
        q[...] = nn(a[...], r.wA[l, 0]).astype(BF16)
        for head in range(2):
            lanes = slice(head * HD, (head + 1) * HD)

            def local(i):
                block = span(i, 128)
                scores = nt(q[block, lanes], k[own, lanes]) * (HD**-0.5)
                row = lax.broadcasted_iota(jnp.int32, (128, SEG), 0) + i * 128
                col = lax.broadcasted_iota(jnp.int32, (128, SEG), 1)
                allowed = (col <= row) & ((col >= bound) | (row < bound))
                r.p[l, head, block, own] = jnp.where(allowed, jnp.exp(scores), 0.0)

            loop(2, local)
        if l == 0:
            bound_copy.wait()
        send_k.wait()
        for head in range(2):
            lanes = slice(head * HD, (head + 1) * HD)

            def memory(i):
                block = span(i, 128)
                scores = nt(q[block, lanes], k[0:SEG, lanes]) * (HD**-0.5)
                row = lax.broadcasted_iota(jnp.int32, (128, SEG), 0) + i * 128
                col = lax.broadcasted_iota(jnp.int32, (128, SEG), 1)
                prior = lax.rem(r.br[0:1, :], SEG)
                allowed = (row < bound) & (restart == 0) & (col >= prior)
                e = jnp.where(allowed, jnp.exp(scores), 0.0)
                e_own = r.p[l, head, block, own]
                total = jnp.sum(e + e_own, axis=-1, keepdims=True)
                r.p[l, head, block, 0:SEG] = e / total
                r.p[l, head, block, own] = e_own / total

            loop(2, memory)
        send_v.wait()
        prev = r.a.at[l, at_rows(core * 128)]
        send_a = remote(
            r.a.at[l, at_rows(SEG + core * 128)],
            prev,
            r.pa_s.at[l, 0],
            r.pa_r.at[l, 0],
            following,
        )
        send_a.start()
        for head in range(2):
            lanes = slice(head * HD, (head + 1) * HD)

            def attend(i):
                block = span(i, 128)
                probs = r.p[l, head, block, :].astype(BF16)
                r.ctx[l, block, lanes] = nn(probs, v[:, lanes]).astype(BF16)

            loop(2, attend)
        loads["O", l].wait()
        copy = ar_begin(
            2 * l, lambda base, i: nt(r.ctx[l, at_rows(base), :], r.wO[l, span(i, 256), :])
        )
        ar_end(2 * l, copy, r.mid.at[l], h)
        norm_into(r.mid.at[l], 2 * l + 1, r.b.at[l])
        loads["U", l].wait()

        def upper(i):
            lanes = span(i, 256)
            u = nn(r.b[l], r.wU[l, :, lanes])
            th = jnp.tanh(ROOT * (u + CUBIC * (u * u * u)))
            half = 0.5 * (1.0 + th)
            r.act[l, :, lanes] = (u * half).astype(BF16)
            r.slope[l, :, lanes] = half + (0.5 * ROOT) * u * (1.0 - th * th) * (
                1.0 + (3.0 * CUBIC) * (u * u)
            )

        loop(4, upper)
        loads["D", l].wait()
        copy = ar_begin(
            2 * l + 1,
            lambda base, i: nt(r.act[l, at_rows(base), :], r.wD[l, span(i, 256), :]),
        )
        send_a.wait()
        share_a = remote(prev, prev, r.pa_s.at[l, 1], r.pa_r.at[l, 1], beside)
        share_a.start()
        ar_end(2 * l + 1, copy, r.h.at[l + 1], r.mid.at[l])
        share_a.wait()

    def transposed(source):
        count = source.shape[0]

        def cols(i):
            lanes = span(i, 256)
            r.xt[lanes, 0:count] = source[:, lanes].T

        loop(4, cols)

    def outer(g, value):
        g[...] = value.astype(BF16).reshape(g.shape)

    def share(index, narrow, color, write):
        return Share(r, here, index, narrow, COLORS[color], write)

    def wide(index, color, left, write):
        unit = share(index, False, color, write)
        outer(unit.g, left())
        unit.advance()
        return unit

    def step(units):
        for unit in units:
            unit.advance()

    def norm_back(source, k, dy_of, add):
        def rows(i):
            block = span(i, 64)
            dx, dg = norm_vjp(source[block, :].astype(F32), r.gains[k : k + 1, :], dy_of(block))
            r.dh[block, :] = (r.dh[block, :] + dx) if add else dx
            r.gg[k] += jnp.sum(dg.reshape(8, 8, D), axis=0)

        loop(4, rows)

    def rounded_dh():
        def rows(i):
            block = span(i, 64)
            r.dy[block, :] = r.dh[block, :].astype(BF16)

        loop(4, rows)

    dq = r.dctx
    loads["H"].wait()
    dq[...] = r.qcot[...].astype(BF16)

    def top(i):
        lanes = span(i, 256)
        r.wide_tmp[:, lanes] = nn(dq[...], r.wH[:, lanes])

    loop(4, top)
    norm_back(r.h.at[2], 4, lambda block: r.wide_tmp[block, :], False)

    def head_grads():
        norm_into(r.h.at[2], 4, r.final)
        r.oe[0:256, :] = nt(r.final[...], r.wH[...])
        transposed(r.final)
        r.hx_copy = remote(r.hx.at[0], r.hx.at[1], r.hx_s, r.hx_r, beside)

        def write(value):
            r.hx[0] = value
            r.hx_copy.start()

        unit = share(0, True, 0, write)
        outer(unit.g, nn(r.xt[:, 0:SEG], dq[:, span(core, 128)]))
        unit.advance()
        return [unit]

    def head_done():
        r.hx_copy.wait()
        r.oe[256:288, span(core, 128)] = r.hx[0]
        r.oe[256:288, span(1 - core, 128)] = r.hx[1]

    def ffn_back(l, n, early=False):
        rounded_dh()
        down = ffn_kind(l, 0) if early else []

        def gate(i):
            lanes = span(i, 256)
            d_active = nn(r.dy[...], r.wD[l, :, lanes])
            r.dup[:, lanes] = (d_active * r.slope[l, :, lanes]).astype(BF16)

        loop(4, gate)
        return down, ar_begin(
            n, lambda base, i: nt(r.dup[at_rows(base), :], r.wU[l, span(i, 256), :])
        )

    def ffn_kind(l, kind):
        left, right, out = ((r.dy, r.act.at[l], 1024), (r.b.at[l], r.dup, 0))[kind]
        transposed(left)
        units = []
        for n in range(4):

            def write(value, base=out + n * 256):
                r.oz[l, :, base : base + 256] = value

            def block(n=n):
                return nn(r.xt[:, 0:SEG], right[:, n * 256 : (n + 1) * 256])

            units.append(wide(l * 12 + kind * 4 + n, n, block, write))
        return units

    def attention_back(l):
        norm_back(r.mid.at[l], 2 * l + 1, lambda block: r.db[block, :].astype(F32), True)
        rounded_dh()
        r.dctx[...] = nn(r.dy[...], r.wO[l]).astype(BF16)
        q, k, v = r.q.at[l], r.k.at[l], r.v.at[l]
        for head in range(2):
            lanes = slice(head * HD, (head + 1) * HD)
            d = r.dctx[:, lanes]
            probs = r.p[l, head]
            d_probs = nt(d, v[:, lanes])
            inner = jnp.sum(d_probs * probs, axis=-1, keepdims=True)
            d_scores = (probs * (d_probs - inner) * (HD**-0.5)).astype(BF16)
            r.dqs[:, lanes] = nn(d_scores, k[:, lanes]).astype(BF16)
            r.dkv[0, :, lanes] = tn(d_scores, q[:, lanes]).astype(BF16)
            r.dkv[1, :, lanes] = tn(probs.astype(BF16), d).astype(BF16)

    def unit_index(l, n):
        return l * 12 + 8 + n

    def out_grads(l):
        transposed(r.dy)

        def write(value):
            r.oz[l, :, 2048:2304] = value

        return [wide(unit_index(l, 3), 3, lambda: nn(r.xt[:, 0:SEG], r.ctx[l]), write)]

    def qkv_grads(l):
        transposed(r.a.at[l])
        units = []
        for n in range(3):

            def write(value, base=2304 + n * 256):
                r.oz[l, :, base : base + 256] = value

            def left(n=n):
                if n:
                    return nn(r.xt[...], r.dkv[n - 1])
                return nn(r.xt[:, SEG:], r.dqs[...])

            units.append(wide(unit_index(l, n), n, left, write))
        return units

    def back_part(l):
        def part(base, i):
            total = nt(r.dqs[at_rows(base), :], r.wA[l, 0, span(i, 256), :])
            for n in (1, 2):
                total = total + nt(
                    r.dkv[n - 1, at_rows(SEG + base), :], r.wA[l, n, span(i, 256), :]
                )
            return total

        return part

    down1, copy = ffn_back(1, 4, True)
    up1 = ffn_kind(1, 1)
    heads = head_grads()
    step(down1)
    ar_end(4, copy, r.db, None)
    attention_back(1)
    copy = ar_begin(5, back_part(1))
    attn1 = out_grads(1) + qkv_grads(1)
    step(up1)
    step(down1)
    step(heads)
    ar_end(5, copy, r.db, None)
    norm_back(r.h.at[1], 2, lambda block: r.db[block, :].astype(F32), True)
    down0, copy = ffn_back(0, 6, True)
    step(up1)
    step(attn1)
    step(heads)
    up0 = ffn_kind(0, 1)
    ar_end(6, copy, r.db, None)
    step(down1)
    step(up1)
    step(attn1)
    attention_back(0)
    attn0 = out_grads(0) + qkv_grads(0)
    step(down0)
    step(heads)

    def normal(i):
        block = span(i, 64)
        x = r.h[0, block, :].astype(F32)
        r.dh[block, :] = x * lax.rsqrt(jnp.mean(x * x, axis=-1, keepdims=True) + EPS)

    loop(4, normal)
    part = back_part(0)
    for half in range(2):

        def gain(i):
            lanes = span(i, 256)
            rows = pl.ds(half * 128, 128)
            value = part(half * 128, i) * r.dh[rows, lanes]
            r.gg[0, :, lanes] += jnp.sum(value.reshape(16, 8, 256), axis=0)

        loop(4, gain)
    copy = remote(r.gg.at[0], r.g0.at[0], r.g0_s.at[0], r.g0_r.at[0], beside)
    copy.start()
    copy.wait()
    r.g0s[...] = r.gg[0] + r.g0[0]
    copy = remote(r.g0s, r.g0.at[1], r.g0_s.at[1], r.g0_r.at[1], across)
    copy.start()
    step(up0)
    copy.wait()
    rows = [jnp.sum(r.g0s[...] + r.g0[1], axis=0, keepdims=True)]
    rows += [jnp.sum(r.gg[n], axis=0, keepdims=True) for n in range(1, 5)]
    table = jnp.concatenate(rows + [jnp.zeros((123, D), F32)], axis=0)

    def write_gains(value):
        r.oe[288:320, 0:128] = value

    unit = share(1, True, 3, write_gains)
    outer(unit.g, table.T)
    unit.advance()
    gain0 = [unit]
    step(down1)
    step(up1)
    step(attn1)
    step(down0)
    step(attn0)
    step(up0)
    step(gain0)
    step(attn1)
    step(down0)
    step(attn0)
    step(up0)
    step(gain0)
    step(down0)
    step(attn0)
    step(up0)
    step(gain0)
    head_done()
    step(attn0)


def finish(oz, oe, values, attn, out, up, down, head, gains):
    values[...] = oe[0:256, :]
    for n in range(3):
        attn[:, n] = oz[:, :, 2304 + n * 256 : 2560 + n * 256]
    out[...] = oz[:, :, 2048:2304]
    up[...] = oz[:, :, 0:1024]
    down[...] = oz[:, :, 1024:2048]
    head[...] = oe[256:288, :]
    gains[...] = oe[288:320, 0:128].T[0:5, :]


def body(tokens, w_attn, w_out, w_up, w_down, w_head, gains, q_cotangent, bounds, resets):
    vmem = pl.BlockSpec(memory_space=pltpu.VMEM)
    smem = pl.BlockSpec(memory_space=pltpu.SMEM)
    anywhere = pl.BlockSpec(memory_space=pl.ANY)
    shapes = [(2, 32, 3072), (320, 256)]
    outs = pl.pallas_call(
        kernel,
        out_shape=[jax.ShapeDtypeStruct(shape, F32) for shape in shapes],
        in_specs=[anywhere] * 6 + [vmem] * 2 + [smem] * 2,
        out_specs=[vmem] * len(shapes),
        scratch_shapes=list(scratch().values()),
        compiler_params=pltpu.CompilerParams(
            collective_id=0, has_side_effects=True, vmem_limit_bytes=67043328
        ),
    )(
        tokens,
        jnp.transpose(w_attn, (0, 2, 1, 3)),
        w_out,
        w_up,
        w_down,
        w_head,
        gains,
        q_cotangent,
        bounds,
        resets,
    )
    shapes = [
        (256, 256),
        (2, 3, 32, 256),
        (2, 32, 256),
        (2, 32, D),
        (2, 32, D),
        (32, 256),
        (5, 32),
    ]
    values, attn, out, up, down, head, gain = pl.pallas_call(
        finish,
        out_shape=[jax.ShapeDtypeStruct(shape, F32) for shape in shapes],
        in_specs=[vmem] * 2,
        out_specs=[vmem] * len(shapes),
    )(*outs)
    return (values, jnp.transpose(attn, (0, 2, 1, 3)), out, up, down, head.T, gain)


def solution(mesh):
    return jax.shard_map(
        body,
        mesh=mesh,
        in_specs=(
            P("seq", None),
            P(None, None, None, "tensor"),
            P(None, None, "tensor"),
            P(None, None, "tensor"),
            P(None, None, "tensor"),
            P(),
            P(),
            P("seq", None),
            P("seq"),
            P("seq"),
        ),
        out_specs=(
            P("seq", None),
            P(None, "seq", None, "tensor"),
            P(None, "seq", "tensor"),
            P(None, "seq", "tensor"),
            P(None, "seq", "tensor"),
            P(None, "seq"),
            P(None, "seq"),
        ),
        check_vma=False,
    )
```
